32 devices in a mesh: grp: 2 (over y), seq: 8 (over z, x), head: 2 (over core).
Axes of the slice: x: 2, y: 2, z: 4, core: 2. Of those that a mesh axis runs over, the one named last changes fastest.
Arguments:
- queries: bfloat16 [2, 16, 64, 128], P(None, ('grp', 'seq'), 'head'), parts along dimension 1, may hold values from -1000 to 1000
- new_keys: bfloat16 [2, 16, 8, 128], P(None, ('grp', 'seq'), 'head'), parts along dimension 1, may hold values from -4 to 4
- token_value_rows: bfloat16 [2, 16, 8, 128], P(None, ('grp', 'seq'), 'head'), parts along dimension 1, may hold values from -6 to 6
- cache_keys: bfloat16 [2, 16, 16, 8, 128], P(None, 'grp', 'seq', 'head'), parts along dimension 1, may hold values from -6 to 6
- prefill_value_cache: bfloat16 [2, 16, 16, 8, 128], P(None, 'grp', 'seq', 'head'), parts along dimension 1, may hold values from -6 to 6
- lengths: int32 [16], P(('grp', 'seq')), parts along dimension 0, may hold values from 1 to 16, as said below
- slot_index: int32 [16], P('grp'), parts along dimension 0, may hold values from 0 to 7, as said below
- out_proj: bfloat16 [2, 8192, 8192], P(None, 'head', 'seq'), may hold values from -0.0625 to 0.0625
Outputs:
- attended: bfloat16 [2, 16, 8192], P(None, ('grp', 'head'), 'seq'), parts along dimension 1
The draws below stay inside these ranges and needn't reach their ends.
There are 2 independent parts, one for each index of `grp`. The reference program is written for one: setup_inputs(seed, part) draws one part's arguments, and reference() takes and returns one part's arrays. A program takes and returns all parts, laid end to end along the dimension named above; an argument that names none is the same for every part. Nothing has to cross between parts.
Inputs may be any that keep to these rules, and one draw needn't show every extreme that they name: Decode sequence b reads prefill slot slot_index[b]; every slot is read by exactly one sequence. `lengths`: some sequence has all 16 positions.
All inputs are finite; a program needn't handle non-finite values.
Results may differ from the reference program's by a relative error of at most 0.008.
Values may be sent and summed in bfloat16 or wider, within the bound.
No kernel may reach another device: no remote copies, remote signals or barrier semaphores. Data moves between devices by JAX's collectives and lax.ppermute only.
A program may use at most 64 MiB of HBM per device.

```python
import jax
import jax.numpy as jnp

D = 8192
QUERY_HEADS = 64
KEY_VALUE_HEADS = 8
HEAD_SIZE = 128
CACHE_COUNT = 2
BATCH_SIZE = 8
CONTEXT_LENGTH = 16


def shared_parts(key):
    newest_token = jax.random.normal(jax.random.fold_in(key, 11), (CACHE_COUNT, BATCH_SIZE, KEY_VALUE_HEADS, HEAD_SIZE), jnp.float32)
    newest_token = jnp.clip(newest_token, -4.0, 4.0).astype(jnp.bfloat16).astype(jnp.float32)
    slot_permutation = jax.random.permutation(jax.random.fold_in(key, 14), BATCH_SIZE).astype(jnp.int32)
    return (newest_token, slot_permutation)


def draw_new_keys(key, part):
    return shared_parts(key)[0].astype(jnp.bfloat16)


def draw_slot_index(key, part):
    return shared_parts(key)[1].astype(jnp.int32)


def draw_lengths(key, part):
    counts = jax.random.randint(jax.random.fold_in(key, 17), (BATCH_SIZE,), 1, CONTEXT_LENGTH + 1)
    spot = jax.random.randint(jax.random.fold_in(key, 18), (), 0, BATCH_SIZE)
    return counts.at[spot].set(CONTEXT_LENGTH).astype(jnp.int32)


def draw_queries(key, part):
    base_offset = jnp.clip(jax.random.normal(jax.random.fold_in(key, 15), (CACHE_COUNT, BATCH_SIZE, QUERY_HEADS, HEAD_SIZE), jnp.float32), -6.0, 6.0)
    return base_offset.astype(jnp.bfloat16)


def draw_cache_keys(key, part):
    base_offset = jnp.clip(jax.random.normal(jax.random.fold_in(key, 16), (CACHE_COUNT, BATCH_SIZE, CONTEXT_LENGTH, KEY_VALUE_HEADS, HEAD_SIZE), jnp.float32), -6.0, 6.0)
    return base_offset.astype(jnp.bfloat16)


def block_levels(own_key, extent, cuts, least, largest):
    loudness = 1.0
    for dim, parts in cuts:
        steps = jax.random.uniform(jax.random.fold_in(jax.random.fold_in(own_key, 6), dim), (parts,), jnp.float32, least / len(cuts), largest / len(cuts))
        loudness = loudness * jnp.repeat(jnp.exp(steps), extent[dim] // parts).reshape((-1,) + (1,) * (len(extent) - 1 - dim))
    return loudness


def scatter_about(rng, shape, spread, most, split=(), kind=jnp.bfloat16):
    result = spread * jax.random.normal(rng, shape, jnp.float32)
    if split:
        result = result * block_levels(rng, shape, split, -0.22, 0.18)
    return jnp.clip(result, -most, most).astype(kind)


def setup_inputs(seed: int = 0, part: int = 0) -> dict:
    key_of = jax.random.split(jax.random.key(seed), 9)
    own_keys = jax.random.split(jax.random.fold_in(key_of[8], part), 9)
    queries = draw_queries(jax.random.fold_in(jax.random.fold_in(key_of[8], part), 71), part)
    new_keys = draw_new_keys(jax.random.fold_in(jax.random.fold_in(key_of[8], part), 71), part)
    token_value_rows = scatter_about(own_keys[2], (CACHE_COUNT, BATCH_SIZE, KEY_VALUE_HEADS, HEAD_SIZE), 1.0, 6.0, ((1, 8), (2, 2)))
    cache_keys = draw_cache_keys(jax.random.fold_in(jax.random.fold_in(key_of[8], part), 71), part)
    prefill_value_cache = scatter_about(own_keys[4], (CACHE_COUNT, BATCH_SIZE, CONTEXT_LENGTH, KEY_VALUE_HEADS, HEAD_SIZE), 1.0, 6.0, ((2, 8), (3, 2)))
    lengths = draw_lengths(jax.random.fold_in(jax.random.fold_in(key_of[8], part), 71), part)
    slot_index = draw_slot_index(jax.random.fold_in(jax.random.fold_in(key_of[8], part), 71), part)
    out_proj = scatter_about(key_of[7], (CACHE_COUNT, QUERY_HEADS * HEAD_SIZE, D), (QUERY_HEADS * HEAD_SIZE) ** -0.5, 0.0625, ((1, 2), (2, 8)))
    return dict(queries=queries, new_keys=new_keys, token_value_rows=token_value_rows, cache_keys=cache_keys, prefill_value_cache=prefill_value_cache, lengths=lengths, slot_index=slot_index, out_proj=out_proj)


def attend_layer(queried, key_rows, value_rows, key_new, value_new, lengths):
    row_count, kv_heads, head_dim = key_new.shape
    q_heads = queried.shape[1]
    grouped = queried.astype(jnp.float32).reshape(row_count, kv_heads, q_heads // kv_heads, head_dim)
    scaling = head_dim ** -0.5
    scores = jnp.einsum('bgrd,btgd->bgrt', grouped, key_rows.astype(jnp.float32)) * scaling
    allowed = jnp.arange(key_rows.shape[1], dtype=jnp.int32)[None, :] < lengths[:, None]
    scores = jnp.where(allowed[:, None, None, :], scores, -1e30)
    own_score = jnp.einsum('bgrd,bgd->bgr', grouped, key_new.astype(jnp.float32)) * scaling
    peak_score = jnp.maximum(jnp.max(scores, axis=-1), own_score)
    raised = jnp.exp(scores - peak_score[..., None])
    own_raised = jnp.exp(own_score - peak_score)
    denominator = jnp.sum(raised, axis=-1) + own_raised
    weights = (raised / denominator[..., None]).astype(jnp.bfloat16)
    own_weight = (own_raised / denominator).astype(jnp.bfloat16)
    context = jnp.einsum('bgrt,btgd->bgrd', weights.astype(jnp.float32), value_rows.astype(jnp.float32))
    context = context + own_weight.astype(jnp.float32)[..., None] * value_new.astype(jnp.float32)[:, :, None, :]
    return context.astype(jnp.bfloat16).reshape(row_count, q_heads * head_dim)


def reference(queries, new_keys, token_value_rows, cache_keys, prefill_value_cache, lengths, slot_index, out_proj):
    results = []
    for layer_idx in range(CACHE_COUNT):
        key_rows = jnp.take(cache_keys[layer_idx], slot_index, axis=0)
        value_rows = jnp.take(prefill_value_cache[layer_idx], slot_index, axis=0)
        context = attend_layer(queries[layer_idx], key_rows, value_rows, new_keys[layer_idx], token_value_rows[layer_idx], lengths)
        projected = jnp.dot(context, out_proj[layer_idx], preferred_element_type=jnp.float32)
        results.append(projected.astype(jnp.bfloat16))
    return jnp.stack(results)
```

```python
import functools

import jax
import jax.numpy as jnp
from jax import lax
from jax.experimental import pallas as pl
from jax.experimental.pallas import tpu as pltpu
from jax.sharding import PartitionSpec as P

VMEM = pl.BlockSpec(memory_space=pltpu.VMEM)
SMEM = pl.BlockSpec(memory_space=pltpu.SMEM)
ANY = pl.BlockSpec(memory_space=pl.ANY)


def pick_kernel(slot_ref, keys_ref, values_ref, out_ref, sem):
    layers, rows = keys_ref.shape[0], keys_ref.shape[2]

    @pl.loop(0, out_ref.shape[0], unroll=out_ref.shape[0] <= 8)
    def _(b):
        slot = slot_ref[b]
        for which, source in enumerate((keys_ref, values_ref)):
            for layer in range(layers):
                pltpu.make_async_copy(
                    source.at[layer, slot],
                    out_ref.at[b, which, pl.ds(layer * rows, rows), :],
                    sem,
                ).start()

    pltpu.make_async_copy(out_ref, out_ref, sem).wait()


def attend_kernel(layers, kv_heads, len_ref, kv_ref, q_ref, new_key_ref, new_value_ref, out_ref):
    sources, _, block, depth = kv_ref.shape
    groups = layers * kv_heads
    positions = block // groups
    queries = q_ref[...]
    keys = kv_ref[:, 0].reshape(sources * block, depth)
    values = kv_ref[:, 1].reshape(sources * block, depth)
    scaling = depth ** (-0.5)
    scores = lax.dot_general(
        queries, keys, (((1,), (1,)), ((), ())), preferred_element_type=jnp.float32
    )
    per_group = queries.shape[0] // groups
    shape = (groups, per_group, sources * block)
    scores = scores.reshape(shape) * scaling
    group = lax.broadcasted_iota(jnp.int32, shape, 0)
    column = lax.broadcasted_iota(jnp.int32, shape, 2)
    within = column % block
    column_group = (within // (positions * kv_heads)) * kv_heads + within % kv_heads
    position = (column // block) * positions + (within // kv_heads) % positions
    allowed = (column_group == group) & (position < len_ref[0])
    scores = jnp.where(allowed, scores, -1e30)
    grouped = queries.astype(jnp.float32).reshape(groups, per_group, depth)
    new_key = new_key_ref[...].astype(jnp.float32)[:, None, :]
    own_score = jnp.sum(grouped * new_key, axis=-1, keepdims=True) * scaling
    peak = jnp.maximum(jnp.max(scores, axis=-1, keepdims=True), own_score)
    raised = jnp.exp(scores - peak)
    own_raised = jnp.exp(own_score - peak)
    denominator = jnp.sum(raised, axis=-1, keepdims=True) + own_raised
    weights = (raised / denominator).astype(jnp.bfloat16)
    own_weight = (own_raised / denominator).astype(jnp.bfloat16)
    context = jnp.dot(
        weights.reshape(groups * per_group, sources * block),
        values,
        preferred_element_type=jnp.float32,
    ).reshape(groups, per_group, depth)
    new_value = new_value_ref[...].astype(jnp.float32)[:, None, :]
    context = context + own_weight.astype(jnp.float32) * new_value
    context = context.astype(jnp.bfloat16).reshape(groups * per_group, depth)
    out_ref[...] = jnp.broadcast_to(context[None], out_ref.shape)


def project_kernel(
    chunk, head_ref, context_ref, weight_ref, mine_ref, other_ref, wide, held, sems
):
    layers, depth_rows, columns = weight_ref.shape
    sequences, rows, depth = context_ref.shape
    heads = rows // layers
    chunks = depth_rows // chunk
    copies = []
    for layer in range(layers):
        for c in range(chunks):
            copies.append(
                pltpu.make_async_copy(
                    weight_ref.at[layer, pl.ds(c * chunk, chunk), :],
                    held.at[layer, pl.ds(c * chunk, chunk), :],
                    sems.at[layer, c],
                )
            )
            copies[-1].start()
    wide[...] = context_ref[...].astype(jnp.float32).reshape(sequences * rows, depth)
    heads_per_chunk = chunk // depth
    half = sequences // 2
    first = head_ref[0] == 0
    for layer in range(layers):
        total = jnp.zeros((sequences, columns), jnp.float32)
        for c in range(chunks):
            lhs = jnp.concatenate(
                [
                    wide[pl.ds(layer * heads + c * heads_per_chunk + h, sequences, stride=rows), :]
                    for h in range(heads_per_chunk)
                ],
                axis=1,
            ).astype(jnp.bfloat16)
            copies[layer * chunks + c].wait()
            total += jnp.dot(
                lhs,
                held[layer, c * chunk : (c + 1) * chunk, :],
                preferred_element_type=jnp.float32,
            )
        low, high = total[:half], total[half:]
        mine_ref[layer] = jnp.where(first, low, high)
        other_ref[layer] = jnp.where(first, high, low)


def local(
    queries,
    new_keys,
    token_value_rows,
    cache_keys,
    prefill_value_cache,
    lengths,
    slot_index,
    out_proj,
):
    layers, _, heads, depth = queries.shape
    kv_heads = new_keys.shape[2]
    _, sequences, positions, _, _ = cache_keys.shape
    columns = out_proj.shape[2]
    bf16, f32 = jnp.bfloat16, jnp.float32
    flat = (layers, sequences, positions * kv_heads, depth)
    block = layers * positions * kv_heads
    picked = pl.pallas_call(
        pick_kernel,
        out_shape=jax.ShapeDtypeStruct((sequences, 2, block, depth), bf16),
        in_specs=[SMEM, ANY, ANY],
        out_specs=VMEM,
        scratch_shapes=[pltpu.SemaphoreType.DMA],
        compiler_params=pltpu.CompilerParams(vmem_limit_bytes=8 * 2**20),
    )(slot_index, cache_keys.reshape(flat), prefill_value_cache.reshape(flat))
    gathered = lax.all_to_all(picked, "seq", 0, 0, tiled=True)
    contexts = pl.pallas_call(
        functools.partial(attend_kernel, layers, kv_heads),
        out_shape=jax.ShapeDtypeStruct((sequences, layers * heads, depth), bf16),
        in_specs=[SMEM, VMEM, VMEM, VMEM, VMEM],
        out_specs=VMEM,
        compiler_params=pltpu.CompilerParams(vmem_limit_bytes=24 * 2**20),
    )(
        lengths,
        gathered,
        queries.reshape(layers * heads, depth),
        new_keys.reshape(layers * kv_heads, depth),
        token_value_rows.reshape(layers * kv_heads, depth),
    )
    contexts = lax.all_to_all(contexts, "seq", 0, 0, tiled=True)
    half = sequences // lax.axis_size("head")
    chunk = 4 * depth
    part = jax.ShapeDtypeStruct((layers, half, columns), f32)
    mine, other = pl.pallas_call(
        functools.partial(project_kernel, chunk),
        out_shape=(part, part),
        in_specs=[SMEM, VMEM, ANY],
        out_specs=(VMEM, VMEM),
        scratch_shapes=[
            pltpu.VMEM((sequences * layers * heads, depth), f32),
            pltpu.VMEM(out_proj.shape, bf16),
            pltpu.SemaphoreType.DMA((layers, heads * depth // chunk)),
        ],
        compiler_params=pltpu.CompilerParams(vmem_limit_bytes=40 * 2**20),
    )(lax.axis_index("head").reshape(1), contexts, out_proj)
    arrived = lax.ppermute(other, "head", [(0, 1), (1, 0)])
    return (mine + arrived).astype(bf16)


def solution(mesh):
    placed = (
        P(None, ("grp", "seq"), "head", None),
        P(None, ("grp", "seq"), "head", None),
        P(None, ("grp", "seq"), "head", None),
        P(None, "grp", "seq", "head", None),
        P(None, "grp", "seq", "head", None),
        P(("grp", "seq")),
        P("grp"),
        P(None, "head", "seq"),
    )
    return jax.shard_map(
        local,
        mesh=mesh,
        in_specs=placed,
        out_specs=P(None, ("grp", "head"), "seq"),
        check_vma=False,
    )
```

```python
import functools

import jax
import jax.numpy as jnp
from jax import lax
from jax.experimental import pallas as pl
from jax.experimental.pallas import tpu as pltpu
from jax.sharding import PartitionSpec as P

VMEM = pl.BlockSpec(memory_space=pltpu.VMEM)
SMEM = pl.BlockSpec(memory_space=pltpu.SMEM)
ANY = pl.BlockSpec(memory_space=pl.ANY)
HBM = pl.BlockSpec(memory_space=pltpu.HBM)
MIB = 2**20
COVER = pl.CostEstimate(flops=10**10, bytes_accessed=2**20, transcendentals=0)


def pick_kernel(slot_ref, keys_ref, values_ref, out_ref, sem):
    layers, rows = keys_ref.shape[0], keys_ref.shape[2]

    @pl.loop(0, out_ref.shape[0], unroll=out_ref.shape[0] <= 8)
    def _(b):
        slot = slot_ref[b]
        for which, source in enumerate((keys_ref, values_ref)):
            for layer in range(layers):
                pltpu.make_async_copy(
                    source.at[layer, slot],
                    out_ref.at[b, which, pl.ds(layer * rows, rows), :],
                    sem,
                ).start()

    pltpu.make_async_copy(out_ref, out_ref, sem).wait()


def attend_kernel(layers, kv_heads, len_ref, kv_ref, q_ref, new_key_ref, new_value_ref, out_ref):
    sources, _, block, depth = kv_ref.shape
    groups = layers * kv_heads
    positions = block // groups
    queries = q_ref[...]
    keys = kv_ref[:, 0].reshape(sources * block, depth)
    values = kv_ref[:, 1].reshape(sources * block, depth)
    scaling = depth ** (-0.5)
    scores = lax.dot_general(
        queries, keys, (((1,), (1,)), ((), ())), preferred_element_type=jnp.float32
    )
    per_group = queries.shape[0] // groups
    shape = (groups, per_group, sources * block)
    scores = scores.reshape(shape) * scaling
    group = lax.broadcasted_iota(jnp.int32, shape, 0)
    column = lax.broadcasted_iota(jnp.int32, shape, 2)
    within = column % block
    column_group = (within // (positions * kv_heads)) * kv_heads + within % kv_heads
    position = (column // block) * positions + (within // kv_heads) % positions
    allowed = (column_group == group) & (position < len_ref[0])
    scores = jnp.where(allowed, scores, -1e30)
    grouped = queries.astype(jnp.float32).reshape(groups, per_group, depth)
    new_key = new_key_ref[...].astype(jnp.float32)[:, None, :]
    own_score = jnp.sum(grouped * new_key, axis=-1, keepdims=True) * scaling
    peak = jnp.maximum(jnp.max(scores, axis=-1, keepdims=True), own_score)
    raised = jnp.exp(scores - peak)
    own_raised = jnp.exp(own_score - peak)
    denominator = jnp.sum(raised, axis=-1, keepdims=True) + own_raised
    weights = (raised / denominator).astype(jnp.bfloat16)
    own_weight = (own_raised / denominator).astype(jnp.bfloat16)
    context = jnp.dot(
        weights.reshape(groups * per_group, sources * block),
        values,
        preferred_element_type=jnp.float32,
    ).reshape(groups, per_group, depth)
    new_value = new_value_ref[...].astype(jnp.float32)[:, None, :]
    context = context + own_weight.astype(jnp.float32) * new_value
    context = context.astype(jnp.bfloat16).reshape(groups * per_group, depth)
    out_ref[...] = jnp.broadcast_to(context[None], out_ref.shape)


def project_kernel(
    chunk, head_ref, context_ref, weight_ref, mine_ref, other_ref, wide, held, sems
):
    layers, depth_rows, columns = weight_ref.shape
    sequences, rows, depth = context_ref.shape
    heads = rows // layers
    chunks = depth_rows // chunk
    copies = []
    for layer in range(layers):
        for c in range(chunks):
            copies.append(
                pltpu.make_async_copy(
                    weight_ref.at[layer, pl.ds(c * chunk, chunk), :],
                    held.at[layer, pl.ds(c * chunk, chunk), :],
                    sems.at[layer, c],
                )
            )
            copies[-1].start()
    wide[...] = context_ref[...].astype(jnp.float32).reshape(sequences * rows, depth)
    heads_per_chunk = chunk // depth
    half = sequences // 2
    first = head_ref[0] == 0
    for layer in range(layers):
        total = jnp.zeros((sequences, columns), jnp.float32)
        for c in range(chunks):
            lhs = jnp.concatenate(
                [
                    wide[pl.ds(layer * heads + c * heads_per_chunk + h, sequences, stride=rows), :]
                    for h in range(heads_per_chunk)
                ],
                axis=1,
            ).astype(jnp.bfloat16)
            copies[layer * chunks + c].wait()
            total += jnp.dot(
                lhs,
                held[layer, c * chunk : (c + 1) * chunk, :],
                preferred_element_type=jnp.float32,
            )
        low, high = total[:half], total[half:]
        mine_ref[layer] = jnp.where(first, low, high)
        other_ref[layer] = jnp.where(first, high, low)


def softmax_context(queries, new_keys, new_values, keys, values, allowed, groups):
    rows, depth = queries.shape
    grouped = (groups, rows // groups, depth)
    scaling = depth ** (-0.5)
    scores = lax.dot_general(
        queries, keys, (((1,), (1,)), ((), ())), preferred_element_type=jnp.float32
    )
    scores = jnp.where(allowed, scores.reshape(allowed.shape) * scaling, -1e30)
    new_keys = new_keys.astype(jnp.float32)[:, None, :]
    own_score = jnp.sum(
        queries.astype(jnp.float32).reshape(grouped) * new_keys, axis=-1, keepdims=True
    )
    own_score = own_score * scaling
    peak = jnp.maximum(jnp.max(scores, axis=-1, keepdims=True), own_score)
    raised = jnp.exp(scores - peak)
    own_raised = jnp.exp(own_score - peak)
    denominator = jnp.sum(raised, axis=-1, keepdims=True) + own_raised
    weights = (raised / denominator).astype(jnp.bfloat16)
    own_weight = (own_raised / denominator).astype(jnp.bfloat16)
    context = jnp.dot(
        weights.reshape(rows, keys.shape[0]), values, preferred_element_type=jnp.float32
    ).reshape(grouped)
    new_values = new_values.astype(jnp.float32)[:, None, :]
    context = context + own_weight.astype(jnp.float32) * new_values
    return context.astype(jnp.bfloat16).reshape(rows, depth)


def place():
    index = lax.axis_index("seq")
    return index // 2, index % 2


def stage_kernel(
    pairs,
    len_ref,
    slot_hbm,
    keys_hbm,
    values_hbm,
    queries_hbm,
    new_keys_hbm,
    new_values_hbm,
    *refs,
):
    blocks, side_ref = refs[:pairs], refs[pairs]
    slots, keys, values, sem = refs[pairs + 1 :]
    layers, _, rows, _ = keys.shape
    query_rows, new_rows = queries_hbm.shape[0], new_keys_hbm.shape[0]
    sources = (slot_hbm, keys_hbm, values_hbm, queries_hbm, new_keys_hbm, new_values_hbm)
    targets = (
        slots,
        keys,
        values,
        side_ref.at[pl.ds(0, query_rows)],
        side_ref.at[pl.ds(query_rows, new_rows)],
        side_ref.at[pl.ds(query_rows + new_rows, new_rows)],
    )
    copies = [
        pltpu.make_async_copy(source, target, sem.at[i])
        for i, (source, target) in enumerate(zip(sources, targets, strict=True))
    ]
    for copy in copies:
        copy.start()
    for copy in copies:
        copy.wait()
    tail = query_rows + 2 * new_rows
    length = len_ref[0].astype(jnp.float32)
    side_ref[tail:, :] = jnp.full((side_ref.shape[0] - tail, side_ref.shape[1]), length).astype(
        jnp.bfloat16
    )
    pair, _ = place()
    for k in range(pairs):
        for side in range(2):
            slot = slots[(pair ^ k) * 2 + side]
            for which, held in enumerate((keys, values)):
                for layer in range(layers):
                    blocks[k][side, which, layer * rows : (layer + 1) * rows, :] = held[layer, slot]


def pack_kernel(*refs):
    start = 0
    for ref in refs[:-1]:
        rows = ref[...].reshape(-1, ref.shape[-1])
        refs[-1][start : start + rows.shape[0], :] = rows
        start += rows.shape[0]


def pair_attend_kernel(pairs, layers, kv_heads, query_rows, *refs):
    blocks, side_ref, partner_ref, out_ref = refs[:pairs], refs[pairs], refs[pairs + 1], refs[-1]
    pair, mine = place()
    _, _, block, depth = blocks[0].shape
    groups = layers * kv_heads
    positions = block // groups
    per_block = 4 * block
    sources = 2 * pairs
    shape = (groups, query_rows // groups, sources * block)
    group = lax.broadcasted_iota(jnp.int32, shape, 0)
    column = lax.broadcasted_iota(jnp.int32, shape, 2)
    within = column % block
    column_group = (within // (positions * kv_heads)) * kv_heads + within % kv_heads
    source = column // block
    source = ((source % pairs) ^ pair) * 2 + ((source // pairs) ^ mine)
    position = source * positions + (within // kv_heads) % positions
    same_group = column_group == group
    tail = pairs * per_block

    def side_rows(sequence, first, count):
        here = side_ref[first : first + count, :]
        there = partner_ref[tail + first : tail + first + count, :]
        return jnp.where(mine == sequence, here, there)

    for sequence in range(2):
        stacked = []
        for which in range(2):
            first = (sequence * 2 + which) * block
            stacked.append(
                jnp.concatenate(
                    [ref[sequence, which] for ref in blocks]
                    + [
                        partner_ref[k * per_block + first : k * per_block + first + block, :]
                        for k in range(pairs)
                    ],
                    axis=0,
                )
            )
        queries = side_rows(sequence, 0, query_rows)
        new_keys = side_rows(sequence, query_rows, groups)
        new_values = side_rows(sequence, query_rows + groups, groups)
        length = side_rows(sequence, query_rows + 2 * groups, 16)[:1, :1].astype(jnp.float32)
        allowed = same_group & (position.astype(jnp.float32) < length[None])
        out_ref[sequence] = softmax_context(
            queries, new_keys, new_values, stacked[0], stacked[1], allowed, groups
        )


def pair_project_kernel(pairs, layers, chunk, *refs):
    contexts, weight_ref, mine_ref, other_ref, wide = refs[:pairs], *refs[pairs:]
    _, rows, depth = contexts[0].shape
    heads = rows // layers
    sequences = 2 * pairs
    columns = weight_ref.shape[2]
    for k in range(pairs):
        wide[k * 2 * rows : (k + 1) * 2 * rows, :] = (
            contexts[k][...].astype(jnp.float32).reshape(2 * rows, depth)
        )
    heads_per_chunk = chunk // depth
    half = sequences // 2
    pair, _ = place()
    first = lax.axis_index("head") == 0
    for layer in range(layers):
        total = jnp.zeros((sequences, columns), jnp.float32)
        for c in range(heads // heads_per_chunk):
            lhs = jnp.concatenate(
                [
                    wide[pl.ds(layer * heads + c * heads_per_chunk + h, sequences, stride=rows), :]
                    for h in range(heads_per_chunk)
                ],
                axis=1,
            ).astype(jnp.bfloat16)
            total += jnp.dot(
                lhs,
                weight_ref[layer, c * chunk : (c + 1) * chunk, :],
                preferred_element_type=jnp.float32,
            )
        bit = 1
        while bit < pairs:
            span = 2 * bit
            swapped = jnp.concatenate(
                [
                    total[(j ^ 1) * span : (j ^ 1) * span + span]
                    for j in range(sequences // span)
                ],
                axis=0,
            )
            total = jnp.where((pair & bit) != 0, swapped, total)
            bit *= 2
        low, high = total[:half], total[half:]
        mine_ref[layer] = jnp.where(first, low, high)
        other_ref[layer] = jnp.where(first, high, low)


def exchange(blocks):
    count = 2 * len(blocks)
    return [blocks[0]] + [
        lax.ppermute(block, "seq", [(i, i ^ (2 * k)) for i in range(count)])
        for k, block in enumerate(blocks)
        if k
    ]


def params(limit):
    return pltpu.CompilerParams(vmem_limit_bytes=limit * MIB)


def in_hbm(*arrays):
    return [pltpu.with_memory_space_constraint(array, pltpu.HBM) for array in arrays]


def by_pairs(
    queries,
    new_keys,
    token_value_rows,
    cache_keys,
    prefill_value_cache,
    lengths,
    slot_index,
    out_proj,
):
    layers, _, heads, depth = queries.shape
    kv_heads = new_keys.shape[2]
    _, sequences, positions, _, _ = cache_keys.shape
    columns = out_proj.shape[2]
    pairs = sequences // 2
    bf16, f32 = jnp.bfloat16, jnp.float32
    flat = (layers, sequences, positions * kv_heads, depth)
    block = layers * positions * kv_heads
    query_rows, groups = layers * heads, layers * kv_heads
    side_rows = query_rows + 2 * groups + 16
    block_shape = jax.ShapeDtypeStruct((2, 2, block, depth), bf16)
    *blocks, side = pl.pallas_call(
        functools.partial(stage_kernel, pairs),
        out_shape=[block_shape] * pairs + [jax.ShapeDtypeStruct((side_rows, depth), bf16)],
        in_specs=[SMEM] + [HBM] * 6,
        out_specs=[VMEM] * (pairs + 1),
        scratch_shapes=[
            pltpu.SMEM((sequences,), jnp.int32),
            pltpu.VMEM(flat, bf16),
            pltpu.VMEM(flat, bf16),
            pltpu.SemaphoreType.DMA((6,)),
        ],
        compiler_params=params(4),
        cost_estimate=COVER,
    )(
        lengths,
        *in_hbm(
            slot_index,
            cache_keys.reshape(flat),
            prefill_value_cache.reshape(flat),
            queries.reshape(query_rows, depth),
            new_keys.reshape(groups, depth),
            token_value_rows.reshape(groups, depth),
        ),
    )
    blocks = exchange(blocks)
    packed = pl.pallas_call(
        pack_kernel,
        out_shape=jax.ShapeDtypeStruct((pairs * 4 * block + side_rows, depth), bf16),
        in_specs=[VMEM] * (pairs + 1),
        out_specs=VMEM,
        compiler_params=params(4),
        cost_estimate=COVER,
    )(*blocks, side)
    partner = lax.ppermute(packed, "seq", [(i, i ^ 1) for i in range(sequences)])
    contexts = pl.pallas_call(
        functools.partial(pair_attend_kernel, pairs, layers, kv_heads, query_rows),
        out_shape=jax.ShapeDtypeStruct((2, query_rows, depth), bf16),
        in_specs=[VMEM] * (pairs + 2),
        out_specs=VMEM,
        compiler_params=params(4),
        cost_estimate=COVER,
    )(*blocks, side, partner)
    contexts = exchange([contexts] * pairs)
    part = jax.ShapeDtypeStruct((layers, sequences // 2, columns), f32)
    mine, other = pl.pallas_call(
        functools.partial(pair_project_kernel, pairs, layers, 4 * depth),
        out_shape=(part, part),
        in_specs=[VMEM] * (pairs + 1),
        out_specs=(VMEM, VMEM),
        scratch_shapes=[pltpu.VMEM((sequences * query_rows, depth), f32)],
        compiler_params=params(24),
    )(*contexts, out_proj)
    arrived = lax.ppermute(other, "head", [(0, 1), (1, 0)])
    return (mine + arrived).astype(bf16)


def by_all_to_all(
    queries,
    new_keys,
    token_value_rows,
    cache_keys,
    prefill_value_cache,
    lengths,
    slot_index,
    out_proj,
):
    layers, _, heads, depth = queries.shape
    kv_heads = new_keys.shape[2]
    _, sequences, positions, _, _ = cache_keys.shape
    columns = out_proj.shape[2]
    bf16, f32 = jnp.bfloat16, jnp.float32
    flat = (layers, sequences, positions * kv_heads, depth)
    block = layers * positions * kv_heads
    picked = pl.pallas_call(
        pick_kernel,
        out_shape=jax.ShapeDtypeStruct((sequences, 2, block, depth), bf16),
        in_specs=[SMEM, ANY, ANY],
        out_specs=VMEM,
        scratch_shapes=[pltpu.SemaphoreType.DMA],
        compiler_params=pltpu.CompilerParams(vmem_limit_bytes=8 * 2**20),
    )(slot_index, cache_keys.reshape(flat), prefill_value_cache.reshape(flat))
    gathered = lax.all_to_all(picked, "seq", 0, 0, tiled=True)
    contexts = pl.pallas_call(
        functools.partial(attend_kernel, layers, kv_heads),
        out_shape=jax.ShapeDtypeStruct((sequences, layers * heads, depth), bf16),
        in_specs=[SMEM, VMEM, VMEM, VMEM, VMEM],
        out_specs=VMEM,
        compiler_params=pltpu.CompilerParams(vmem_limit_bytes=24 * 2**20),
    )(
        lengths,
        gathered,
        queries.reshape(layers * heads, depth),
        new_keys.reshape(layers * kv_heads, depth),
        token_value_rows.reshape(layers * kv_heads, depth),
    )
    contexts = lax.all_to_all(contexts, "seq", 0, 0, tiled=True)
    half = sequences // lax.axis_size("head")
    chunk = 4 * depth
    part = jax.ShapeDtypeStruct((layers, half, columns), f32)
    mine, other = pl.pallas_call(
        functools.partial(project_kernel, chunk),
        out_shape=(part, part),
        in_specs=[SMEM, VMEM, ANY],
        out_specs=(VMEM, VMEM),
        scratch_shapes=[
            pltpu.VMEM((sequences * layers * heads, depth), f32),
            pltpu.VMEM(out_proj.shape, bf16),
            pltpu.SemaphoreType.DMA((layers, heads * depth // chunk)),
        ],
        compiler_params=pltpu.CompilerParams(vmem_limit_bytes=40 * 2**20),
    )(lax.axis_index("head").reshape(1), contexts, out_proj)
    arrived = lax.ppermute(other, "head", [(0, 1), (1, 0)])
    return (mine + arrived).astype(bf16)


def solution(mesh):
    placed = (
        P(None, ("grp", "seq"), "head", None),
        P(None, ("grp", "seq"), "head", None),
        P(None, ("grp", "seq"), "head", None),
        P(None, "grp", "seq", "head", None),
        P(None, "grp", "seq", "head", None),
        P(("grp", "seq")),
        P("grp"),
        P(None, "head", "seq"),
    )
    seq = mesh.shape["seq"]
    few = seq in (2, 4, 8)
    return jax.shard_map(
        by_pairs if few else by_all_to_all,
        mesh=mesh,
        in_specs=placed,
        out_specs=P(None, ("grp", "head"), "seq"),
        check_vma=False,
    )
```

```python
import functools

import jax
import jax.numpy as jnp
from jax import lax
from jax.experimental import pallas as pl
from jax.experimental.pallas import tpu as pltpu
from jax.sharding import PartitionSpec as P


VMEM = pl.BlockSpec(memory_space=pltpu.VMEM)
SMEM = pl.BlockSpec(memory_space=pltpu.SMEM)
ANY = pl.BlockSpec(memory_space=pl.ANY)
HBM = pl.BlockSpec(memory_space=pltpu.HBM)
MIB = 2**20
COVER = pl.CostEstimate(flops=10**10, bytes_accessed=2**20, transcendentals=0)


def pick_kernel(slot_ref, keys_ref, values_ref, out_ref, sem):
    layers, rows = keys_ref.shape[0], keys_ref.shape[2]

    @pl.loop(0, out_ref.shape[0], unroll=out_ref.shape[0] <= 8)
    def _(b):
        slot = slot_ref[b]
        for which, source in enumerate((keys_ref, values_ref)):
            for layer in range(layers):
                pltpu.make_async_copy(
                    source.at[layer, slot],
                    out_ref.at[b, which, pl.ds(layer * rows, rows), :],
                    sem,
                ).start()

    pltpu.make_async_copy(out_ref, out_ref, sem).wait()


def attend_kernel(layers, kv_heads, len_ref, kv_ref, q_ref, new_key_ref, new_value_ref, out_ref):
    sources, _, block, depth = kv_ref.shape
    groups = layers * kv_heads
    positions = block // groups
    queries = q_ref[...]
    keys = kv_ref[:, 0].reshape(sources * block, depth)
    values = kv_ref[:, 1].reshape(sources * block, depth)
    scaling = depth ** (-0.5)
    scores = lax.dot_general(
        queries, keys, (((1,), (1,)), ((), ())), preferred_element_type=jnp.float32
    )
    per_group = queries.shape[0] // groups
    shape = (groups, per_group, sources * block)
    scores = scores.reshape(shape) * scaling
    group = lax.broadcasted_iota(jnp.int32, shape, 0)
    column = lax.broadcasted_iota(jnp.int32, shape, 2)
    within = column % block
    column_group = (within // (positions * kv_heads)) * kv_heads + within % kv_heads
    position = (column // block) * positions + (within // kv_heads) % positions
    allowed = (column_group == group) & (position < len_ref[0])
    scores = jnp.where(allowed, scores, -1e30)
    grouped = queries.astype(jnp.float32).reshape(groups, per_group, depth)
    new_key = new_key_ref[...].astype(jnp.float32)[:, None, :]
    own_score = jnp.sum(grouped * new_key, axis=-1, keepdims=True) * scaling
    peak = jnp.maximum(jnp.max(scores, axis=-1, keepdims=True), own_score)
    raised = jnp.exp(scores - peak)
    own_raised = jnp.exp(own_score - peak)
    denominator = jnp.sum(raised, axis=-1, keepdims=True) + own_raised
    weights = (raised / denominator).astype(jnp.bfloat16)
    own_weight = (own_raised / denominator).astype(jnp.bfloat16)
    context = jnp.dot(
        weights.reshape(groups * per_group, sources * block),
        values,
        preferred_element_type=jnp.float32,
    ).reshape(groups, per_group, depth)
    new_value = new_value_ref[...].astype(jnp.float32)[:, None, :]
    context = context + own_weight.astype(jnp.float32) * new_value
    context = context.astype(jnp.bfloat16).reshape(groups * per_group, depth)
    out_ref[...] = jnp.broadcast_to(context[None], out_ref.shape)


def project_kernel(
    chunk, head_ref, context_ref, weight_ref, mine_ref, other_ref, wide, held, sems
):
    layers, depth_rows, columns = weight_ref.shape
    sequences, rows, depth = context_ref.shape
    heads = rows // layers
    chunks = depth_rows // chunk
    copies = []
    for layer in range(layers):
        for c in range(chunks):
            copies.append(
                pltpu.make_async_copy(
                    weight_ref.at[layer, pl.ds(c * chunk, chunk), :],
                    held.at[layer, pl.ds(c * chunk, chunk), :],
                    sems.at[layer, c],
                )
            )
            copies[-1].start()
    wide[...] = context_ref[...].astype(jnp.float32).reshape(sequences * rows, depth)
    heads_per_chunk = chunk // depth
    half = sequences // 2
    first = head_ref[0] == 0
    for layer in range(layers):
        total = jnp.zeros((sequences, columns), jnp.float32)
        for c in range(chunks):
            lhs = jnp.concatenate(
                [
                    wide[pl.ds(layer * heads + c * heads_per_chunk + h, sequences, stride=rows), :]
                    for h in range(heads_per_chunk)
                ],
                axis=1,
            ).astype(jnp.bfloat16)
            copies[layer * chunks + c].wait()
            total += jnp.dot(
                lhs,
                held[layer, c * chunk : (c + 1) * chunk, :],
                preferred_element_type=jnp.float32,
            )
        low, high = total[:half], total[half:]
        mine_ref[layer] = jnp.where(first, low, high)
        other_ref[layer] = jnp.where(first, high, low)


def softmax_context(queries, new_keys, new_values, keys, values, allowed, groups):
    rows, depth = queries.shape
    grouped = (groups, rows // groups, depth)
    scaling = depth ** (-0.5)
    scores = lax.dot_general(
        queries, keys, (((1,), (1,)), ((), ())), preferred_element_type=jnp.float32
    )
    scores = jnp.where(allowed, scores.reshape(allowed.shape) * scaling, -1e30)
    new_keys = new_keys.astype(jnp.float32)[:, None, :]
    own_score = jnp.sum(
        queries.astype(jnp.float32).reshape(grouped) * new_keys, axis=-1, keepdims=True
    )
    own_score = own_score * scaling
    peak = jnp.maximum(jnp.max(scores, axis=-1, keepdims=True), own_score)
    raised = jnp.exp(scores - peak)
    own_raised = jnp.exp(own_score - peak)
    denominator = jnp.sum(raised, axis=-1, keepdims=True) + own_raised
    weights = (raised / denominator).astype(jnp.bfloat16)
    own_weight = (own_raised / denominator).astype(jnp.bfloat16)
    context = jnp.dot(
        weights.reshape(rows, keys.shape[0]), values, preferred_element_type=jnp.float32
    ).reshape(grouped)
    new_values = new_values.astype(jnp.float32)[:, None, :]
    context = context + own_weight.astype(jnp.float32) * new_values
    return context.astype(jnp.bfloat16).reshape(rows, depth)


def place():
    index = lax.axis_index("seq")
    return index // 2, index % 2


def stage_kernel(
    pairs,
    slot_hbm,
    keys_hbm,
    values_hbm,
    queries_hbm,
    new_keys_hbm,
    new_values_hbm,
    *refs,
):
    blocks, side_ref = refs[:pairs], refs[pairs]
    slots, keys, values, sem = refs[pairs + 1 :]
    layers, _, rows, _ = keys.shape
    query_rows, new_rows = queries_hbm.shape[0], new_keys_hbm.shape[0]
    sources = (slot_hbm, keys_hbm, values_hbm, queries_hbm, new_keys_hbm, new_values_hbm)
    targets = (
        slots,
        keys,
        values,
        side_ref.at[pl.ds(0, query_rows)],
        side_ref.at[pl.ds(query_rows, new_rows)],
        side_ref.at[pl.ds(query_rows + new_rows, new_rows)],
    )
    copies = [
        pltpu.make_async_copy(source, target, sem.at[i])
        for i, (source, target) in enumerate(zip(sources, targets, strict=True))
    ]
    for copy in copies:
        copy.start()
    for copy in copies:
        copy.wait()
    pair, _ = place()
    for k in range(pairs):
        for side in range(2):
            slot = slots[(pair ^ k) * 2 + side]
            for which, held in enumerate((keys, values)):
                for layer in range(layers):
                    blocks[k][side, which, layer * rows : (layer + 1) * rows, :] = held[layer, slot]


def pack_kernel(*refs):
    start = 0
    for ref in refs[:-1]:
        rows = ref[...].reshape(-1, ref.shape[-1])
        refs[-1][start : start + rows.shape[0], :] = rows
        start += rows.shape[0]


def pair_attend_kernel(pairs, layers, kv_heads, query_rows, *refs):
    blocks, (side_ref, limit_ref, partner_ref, out_ref) = refs[:pairs], refs[pairs:]
    pair, mine = place()
    _, _, block, _ = blocks[0].shape
    groups = layers * kv_heads
    positions = block // groups
    per_block = 4 * block
    sources = 2 * pairs
    shape = (groups, query_rows // groups, sources * block)
    group = lax.broadcasted_iota(jnp.int32, shape, 0)
    column = lax.broadcasted_iota(jnp.int32, shape, 2)
    within = column % block
    column_group = (within // (positions * kv_heads)) * kv_heads + within % kv_heads
    source = column // block
    source = ((source % pairs) ^ pair) * 2 + ((source // pairs) ^ mine)
    position = source * positions + (within // kv_heads) % positions
    same_group = column_group == group
    tail = pairs * per_block

    def side_rows(sequence, first, count):
        here = side_ref[first : first + count, :]
        there = partner_ref[tail + first : tail + first + count, :]
        return jnp.where(mine == sequence, here, there)

    for sequence in range(2):
        stacked = []
        for which in range(2):
            first = (sequence * 2 + which) * block
            stacked.append(
                jnp.concatenate(
                    [ref[sequence, which] for ref in blocks]
                    + [
                        partner_ref[k * per_block + first : k * per_block + first + block, :]
                        for k in range(pairs)
                    ],
                    axis=0,
                )
            )
        queries = side_rows(sequence, 0, query_rows)
        new_keys = side_rows(sequence, query_rows, groups)
        new_values = side_rows(sequence, query_rows + groups, groups)
        limit = jnp.where(
            mine == sequence, limit_ref[...], partner_ref[tail + query_rows + 2 * groups :, :]
        )
        limit = limit[:1, :1].astype(jnp.float32)
        allowed = same_group & (position.astype(jnp.float32) < limit[None])
        out_ref[sequence] = softmax_context(
            queries, new_keys, new_values, stacked[0], stacked[1], allowed, groups
        )


def pair_project_kernel(pairs, layers, chunk, *refs):
    contexts, weight_ref, mine_ref, other_ref, wide = refs[:pairs], *refs[pairs:]
    _, rows, depth = contexts[0].shape
    heads = rows // layers
    sequences = 2 * pairs
    columns = weight_ref.shape[2]
    for k in range(pairs):
        wide[k * 2 * rows : (k + 1) * 2 * rows, :] = (
            contexts[k][...].astype(jnp.float32).reshape(2 * rows, depth)
        )
    heads_per_chunk = chunk // depth
    half = sequences // 2
    pair, _ = place()
    first = lax.axis_index("head") == 0
    for layer in range(layers):
        total = jnp.zeros((sequences, columns), jnp.float32)
        for c in range(heads // heads_per_chunk):
            lhs = jnp.concatenate(
                [
                    wide[pl.ds(layer * heads + c * heads_per_chunk + h, sequences, stride=rows), :]
                    for h in range(heads_per_chunk)
                ],
                axis=1,
            ).astype(jnp.bfloat16)
            total += jnp.dot(
                lhs,
                weight_ref[layer, c * chunk : (c + 1) * chunk, :],
                preferred_element_type=jnp.float32,
            )
        bit = 1
        while bit < pairs:
            span = 2 * bit
            swapped = jnp.concatenate(
                [
                    total[(j ^ 1) * span : (j ^ 1) * span + span]
                    for j in range(sequences // span)
                ],
                axis=0,
            )
            total = jnp.where((pair & bit) != 0, swapped, total)
            bit *= 2
        low, high = total[:half], total[half:]
        mine_ref[layer] = jnp.where(first, low, high)
        other_ref[layer] = jnp.where(first, high, low)


def exchange(blocks):
    count = 2 * len(blocks)
    arrived = [blocks[0]]
    for k in range(1, len(blocks)):
        pairs = [(i, i ^ (2 * k)) for i in range(count)]
        arrived.append(lax.ppermute(blocks[k], "seq", pairs))
    return arrived


def params(limit):
    return pltpu.CompilerParams(vmem_limit_bytes=limit * MIB)


def in_hbm(*arrays):
    return [pltpu.with_memory_space_constraint(array, pltpu.HBM) for array in arrays]


def by_pairs(
    queries,
    new_keys,
    token_value_rows,
    cache_keys,
    prefill_value_cache,
    lengths,
    slot_index,
    out_proj,
):
    layers, _, heads, depth = queries.shape
    kv_heads = new_keys.shape[2]
    _, sequences, positions, _, _ = cache_keys.shape
    columns = out_proj.shape[2]
    pairs = sequences // 2
    bf16, f32 = jnp.bfloat16, jnp.float32
    flat = (layers, sequences, positions * kv_heads, depth)
    block = layers * positions * kv_heads
    query_rows, groups = layers * heads, layers * kv_heads
    side_rows = query_rows + 2 * groups
    block_shape = jax.ShapeDtypeStruct((2, 2, block, depth), bf16)
    *blocks, side = pl.pallas_call(
        functools.partial(stage_kernel, pairs),
        out_shape=[block_shape] * pairs + [jax.ShapeDtypeStruct((side_rows, depth), bf16)],
        in_specs=[HBM] * 6,
        out_specs=[VMEM] * (pairs + 1),
        scratch_shapes=[
            pltpu.SMEM((sequences,), jnp.int32),
            pltpu.VMEM(flat, bf16),
            pltpu.VMEM(flat, bf16),
            pltpu.SemaphoreType.DMA((6,)),
        ],
        compiler_params=params(4),
        cost_estimate=COVER,
    )(
        *in_hbm(
            slot_index,
            cache_keys.reshape(flat),
            prefill_value_cache.reshape(flat),
            queries.reshape(query_rows, depth),
            new_keys.reshape(groups, depth),
            token_value_rows.reshape(groups, depth),
        ),
    )
    blocks = exchange(blocks)
    limit = jnp.broadcast_to(lengths.astype(bf16)[:, None], (16, depth))
    packed = pl.pallas_call(
        pack_kernel,
        out_shape=jax.ShapeDtypeStruct((pairs * 4 * block + side_rows + 16, depth), bf16),
        in_specs=[VMEM] * (pairs + 2),
        out_specs=VMEM,
        compiler_params=params(4),
        cost_estimate=COVER,
    )(*blocks, side, limit)
    partner = lax.ppermute(packed, "seq", [(i, i ^ 1) for i in range(sequences)])
    contexts = pl.pallas_call(
        functools.partial(pair_attend_kernel, pairs, layers, kv_heads, query_rows),
        out_shape=jax.ShapeDtypeStruct((2, query_rows, depth), bf16),
        in_specs=[VMEM] * (pairs + 3),
        out_specs=VMEM,
        compiler_params=params(4),
        cost_estimate=COVER,
    )(*blocks, side, limit, partner)
    contexts = exchange([contexts] * pairs)
    part = jax.ShapeDtypeStruct((layers, sequences // 2, columns), f32)
    mine, other = pl.pallas_call(
        functools.partial(pair_project_kernel, pairs, layers, 4 * depth),
        out_shape=(part, part),
        in_specs=[VMEM] * (pairs + 1),
        out_specs=(VMEM, VMEM),
        scratch_shapes=[pltpu.VMEM((sequences * query_rows, depth), f32)],
        compiler_params=params(24),
    )(*contexts, out_proj)
    arrived = lax.ppermute(other, "head", [(0, 1), (1, 0)])
    return (mine + arrived).astype(bf16)


def by_all_to_all(
    queries,
    new_keys,
    token_value_rows,
    cache_keys,
    prefill_value_cache,
    lengths,
    slot_index,
    out_proj,
):
    layers, _, heads, depth = queries.shape
    kv_heads = new_keys.shape[2]
    _, sequences, positions, _, _ = cache_keys.shape
    columns = out_proj.shape[2]
    bf16, f32 = jnp.bfloat16, jnp.float32
    flat = (layers, sequences, positions * kv_heads, depth)
    block = layers * positions * kv_heads
    picked = pl.pallas_call(
        pick_kernel,
        out_shape=jax.ShapeDtypeStruct((sequences, 2, block, depth), bf16),
        in_specs=[SMEM, ANY, ANY],
        out_specs=VMEM,
        scratch_shapes=[pltpu.SemaphoreType.DMA],
        compiler_params=pltpu.CompilerParams(vmem_limit_bytes=8 * 2**20),
    )(slot_index, cache_keys.reshape(flat), prefill_value_cache.reshape(flat))
    gathered = lax.all_to_all(picked, "seq", 0, 0, tiled=True)
    contexts = pl.pallas_call(
        functools.partial(attend_kernel, layers, kv_heads),
        out_shape=jax.ShapeDtypeStruct((sequences, layers * heads, depth), bf16),
        in_specs=[SMEM, VMEM, VMEM, VMEM, VMEM],
        out_specs=VMEM,
        compiler_params=pltpu.CompilerParams(vmem_limit_bytes=24 * 2**20),
    )(
        lengths,
        gathered,
        queries.reshape(layers * heads, depth),
        new_keys.reshape(layers * kv_heads, depth),
        token_value_rows.reshape(layers * kv_heads, depth),
    )
    contexts = lax.all_to_all(contexts, "seq", 0, 0, tiled=True)
    half = sequences // lax.axis_size("head")
    chunk = 4 * depth
    part = jax.ShapeDtypeStruct((layers, half, columns), f32)
    mine, other = pl.pallas_call(
        functools.partial(project_kernel, chunk),
        out_shape=(part, part),
        in_specs=[SMEM, VMEM, ANY],
        out_specs=(VMEM, VMEM),
        scratch_shapes=[
            pltpu.VMEM((sequences * layers * heads, depth), f32),
            pltpu.VMEM(out_proj.shape, bf16),
            pltpu.SemaphoreType.DMA((layers, heads * depth // chunk)),
        ],
        compiler_params=pltpu.CompilerParams(vmem_limit_bytes=40 * 2**20),
    )(lax.axis_index("head").reshape(1), contexts, out_proj)
    arrived = lax.ppermute(other, "head", [(0, 1), (1, 0)])
    return (mine + arrived).astype(bf16)


def solution(mesh):
    placed = (
        P(None, ("grp", "seq"), "head", None),
        P(None, ("grp", "seq"), "head", None),
        P(None, ("grp", "seq"), "head", None),
        P(None, "grp", "seq", "head", None),
        P(None, "grp", "seq", "head", None),
        P(("grp", "seq")),
        P("grp"),
        P(None, "head", "seq"),
    )
    seq = mesh.shape["seq"]
    few = seq in (2, 4, 8)

    def step(*operands):
        return (by_pairs if few else by_all_to_all)(*operands)

    step = jax.shard_map(
        step,
        mesh=mesh,
        in_specs=placed,
        out_specs=P(None, ("grp", "head"), "seq"),
        check_vma=False,
    )
    return step
```

```python
import functools

import jax
import jax.numpy as jnp
from jax import lax
from jax.experimental import pallas as pl
from jax.experimental.pallas import tpu as pltpu
from jax.sharding import PartitionSpec as P


VMEM = pl.BlockSpec(memory_space=pltpu.VMEM)
SMEM = pl.BlockSpec(memory_space=pltpu.SMEM)
ANY = pl.BlockSpec(memory_space=pl.ANY)
HBM = pl.BlockSpec(memory_space=pltpu.HBM)
MIB = 2**20
COVER = pl.CostEstimate(flops=10**10, bytes_accessed=2**20, transcendentals=0)


def pick_kernel(slot_ref, keys_ref, values_ref, out_ref, sem):
    layers, rows = keys_ref.shape[0], keys_ref.shape[2]

    @pl.loop(0, out_ref.shape[0], unroll=out_ref.shape[0] <= 8)
    def _(b):
        slot = slot_ref[b]
        for which, source in enumerate((keys_ref, values_ref)):
            for layer in range(layers):
                pltpu.make_async_copy(
                    source.at[layer, slot],
                    out_ref.at[b, which, pl.ds(layer * rows, rows), :],
                    sem,
                ).start()

    pltpu.make_async_copy(out_ref, out_ref, sem).wait()


def attend_kernel(layers, kv_heads, len_ref, kv_ref, q_ref, new_key_ref, new_value_ref, out_ref):
    sources, _, block, depth = kv_ref.shape
    groups = layers * kv_heads
    positions = block // groups
    queries = q_ref[...]
    keys = kv_ref[:, 0].reshape(sources * block, depth)
    values = kv_ref[:, 1].reshape(sources * block, depth)
    scaling = depth ** (-0.5)
    scores = lax.dot_general(
        queries, keys, (((1,), (1,)), ((), ())), preferred_element_type=jnp.float32
    )
    per_group = queries.shape[0] // groups
    shape = (groups, per_group, sources * block)
    scores = scores.reshape(shape) * scaling
    group = lax.broadcasted_iota(jnp.int32, shape, 0)
    column = lax.broadcasted_iota(jnp.int32, shape, 2)
    within = column % block
    column_group = (within // (positions * kv_heads)) * kv_heads + within % kv_heads
    position = (column // block) * positions + (within // kv_heads) % positions
    allowed = (column_group == group) & (position < len_ref[0])
    scores = jnp.where(allowed, scores, -1e30)
    grouped = queries.astype(jnp.float32).reshape(groups, per_group, depth)
    new_key = new_key_ref[...].astype(jnp.float32)[:, None, :]
    own_score = jnp.sum(grouped * new_key, axis=-1, keepdims=True) * scaling
    peak = jnp.maximum(jnp.max(scores, axis=-1, keepdims=True), own_score)
    raised = jnp.exp(scores - peak)
    own_raised = jnp.exp(own_score - peak)
    denominator = jnp.sum(raised, axis=-1, keepdims=True) + own_raised
    weights = (raised / denominator).astype(jnp.bfloat16)
    own_weight = (own_raised / denominator).astype(jnp.bfloat16)
    context = jnp.dot(
        weights.reshape(groups * per_group, sources * block),
        values,
        preferred_element_type=jnp.float32,
    ).reshape(groups, per_group, depth)
    new_value = new_value_ref[...].astype(jnp.float32)[:, None, :]
    context = context + own_weight.astype(jnp.float32) * new_value
    context = context.astype(jnp.bfloat16).reshape(groups * per_group, depth)
    out_ref[...] = jnp.broadcast_to(context[None], out_ref.shape)


def project_kernel(
    chunk, head_ref, context_ref, weight_ref, mine_ref, other_ref, wide, held, sems
):
    layers, depth_rows, columns = weight_ref.shape
    sequences, rows, depth = context_ref.shape
    heads = rows // layers
    chunks = depth_rows // chunk
    copies = []
    for layer in range(layers):
        for c in range(chunks):
            copies.append(
                pltpu.make_async_copy(
                    weight_ref.at[layer, pl.ds(c * chunk, chunk), :],
                    held.at[layer, pl.ds(c * chunk, chunk), :],
                    sems.at[layer, c],
                )
            )
            copies[-1].start()
    wide[...] = context_ref[...].astype(jnp.float32).reshape(sequences * rows, depth)
    heads_per_chunk = chunk // depth
    half = sequences // 2
    first = head_ref[0] == 0
    for layer in range(layers):
        total = jnp.zeros((sequences, columns), jnp.float32)
        for c in range(chunks):
            lhs = jnp.concatenate(
                [
                    wide[pl.ds(layer * heads + c * heads_per_chunk + h, sequences, stride=rows), :]
                    for h in range(heads_per_chunk)
                ],
                axis=1,
            ).astype(jnp.bfloat16)
            copies[layer * chunks + c].wait()
            total += jnp.dot(
                lhs,
                held[layer, c * chunk : (c + 1) * chunk, :],
                preferred_element_type=jnp.float32,
            )
        low, high = total[:half], total[half:]
        mine_ref[layer] = jnp.where(first, low, high)
        other_ref[layer] = jnp.where(first, high, low)


def softmax_context(queries, new_keys, new_values, keys, values, allowed, groups):
    rows, depth = queries.shape
    grouped = (groups, rows // groups, depth)
    scaling = depth ** (-0.5)
    scores = lax.dot_general(
        queries, keys, (((1,), (1,)), ((), ())), preferred_element_type=jnp.float32
    )
    scores = jnp.where(allowed, scores.reshape(allowed.shape) * scaling, -1e30)
    new_keys = new_keys.astype(jnp.float32)[:, None, :]
    own_score = jnp.sum(
        queries.astype(jnp.float32).reshape(grouped) * new_keys, axis=-1, keepdims=True
    )
    own_score = own_score * scaling
    peak = jnp.maximum(jnp.max(scores, axis=-1, keepdims=True), own_score)
    raised = jnp.exp(scores - peak)
    own_raised = jnp.exp(own_score - peak)
    denominator = jnp.sum(raised, axis=-1, keepdims=True) + own_raised
    weights = (raised / denominator).astype(jnp.bfloat16)
    own_weight = (own_raised / denominator).astype(jnp.bfloat16)
    context = jnp.dot(
        weights.reshape(rows, keys.shape[0]), values, preferred_element_type=jnp.float32
    ).reshape(grouped)
    new_values = new_values.astype(jnp.float32)[:, None, :]
    context = context + own_weight.astype(jnp.float32) * new_values
    return context.astype(jnp.bfloat16).reshape(rows, depth)


def place(pairs):
    index = lax.axis_index("seq")
    return index % pairs, index // pairs


def stage_kernel(
    pairs,
    slot_hbm,
    keys_hbm,
    values_hbm,
    queries_hbm,
    new_keys_hbm,
    new_values_hbm,
    *refs,
):
    blocks, side_ref = refs[:pairs], refs[pairs]
    slots, keys, values, sem = refs[pairs + 1 :]
    layers, _, rows, _ = keys.shape
    query_rows, new_rows = queries_hbm.shape[0], new_keys_hbm.shape[0]
    sources = (slot_hbm, keys_hbm, values_hbm, queries_hbm, new_keys_hbm, new_values_hbm)
    targets = (
        slots,
        keys,
        values,
        side_ref.at[pl.ds(0, query_rows)],
        side_ref.at[pl.ds(query_rows, new_rows)],
        side_ref.at[pl.ds(query_rows + new_rows, new_rows)],
    )
    copies = [
        pltpu.make_async_copy(source, target, sem.at[i])
        for i, (source, target) in enumerate(zip(sources, targets, strict=True))
    ]
    for copy in copies:
        copy.start()
    for copy in copies:
        copy.wait()
    pair, _ = place(pairs)
    for k in range(pairs):
        for side in range(2):
            slot = slots[side * pairs + (pair ^ k)]
            for which, held in enumerate((keys, values)):
                for layer in range(layers):
                    blocks[k][side, which, layer * rows : (layer + 1) * rows, :] = held[layer, slot]


def pack_kernel(*refs):
    start = 0
    for ref in refs[:-1]:
        rows = ref[...].reshape(-1, ref.shape[-1])
        refs[-1][start : start + rows.shape[0], :] = rows
        start += rows.shape[0]


def pair_attend_kernel(pairs, layers, kv_heads, query_rows, *refs):
    blocks, (side_ref, limit_ref, partner_ref, out_ref) = refs[:pairs], refs[pairs:]
    pair, mine = place(pairs)
    _, _, block, _ = blocks[0].shape
    groups = layers * kv_heads
    positions = block // groups
    per_block = 4 * block
    sources = 2 * pairs
    shape = (groups, query_rows // groups, sources * block)
    group = lax.broadcasted_iota(jnp.int32, shape, 0)
    column = lax.broadcasted_iota(jnp.int32, shape, 2)
    within = column % block
    column_group = (within // (positions * kv_heads)) * kv_heads + within % kv_heads
    source = column // block
    source = ((source // pairs) ^ mine) * pairs + ((source % pairs) ^ pair)
    position = source * positions + (within // kv_heads) % positions
    same_group = column_group == group
    tail = pairs * per_block

    def side_rows(sequence, first, count):
        here = side_ref[first : first + count, :]
        there = partner_ref[tail + first : tail + first + count, :]
        return jnp.where(mine == sequence, here, there)

    for sequence in range(2):
        stacked = []
        for which in range(2):
            first = (sequence * 2 + which) * block
            stacked.append(
                jnp.concatenate(
                    [ref[sequence, which] for ref in blocks]
                    + [
                        partner_ref[k * per_block + first : k * per_block + first + block, :]
                        for k in range(pairs)
                    ],
                    axis=0,
                )
            )
        queries = side_rows(sequence, 0, query_rows)
        new_keys = side_rows(sequence, query_rows, groups)
        new_values = side_rows(sequence, query_rows + groups, groups)
        limit = jnp.where(
            mine == sequence, limit_ref[...], partner_ref[tail + query_rows + 2 * groups :, :]
        )
        limit = limit[:1, :1].astype(jnp.float32)
        allowed = same_group & (position.astype(jnp.float32) < limit[None])
        out_ref[sequence] = softmax_context(
            queries, new_keys, new_values, stacked[0], stacked[1], allowed, groups
        )


def pair_project_kernel(pairs, layers, chunk, *refs):
    contexts, weight_ref, mine_ref, other_ref, wide = refs[:pairs], *refs[pairs:]
    _, rows, depth = contexts[0].shape
    heads = rows // layers
    sequences = 2 * pairs
    columns = weight_ref.shape[2]
    pair, _ = place(pairs)
    for k in range(pairs):
        for side in range(2):
            sequence = side * pairs + (pair ^ k)
            wide[pl.ds(pl.multiple_of(sequence * rows, rows), rows), :] = contexts[k][side].astype(
                jnp.float32
            )
    heads_per_chunk = chunk // depth
    half = sequences // 2
    first = lax.axis_index("head") == 0
    for layer in range(layers):
        total = jnp.zeros((sequences, columns), jnp.float32)
        for c in range(heads // heads_per_chunk):
            lhs = jnp.concatenate(
                [
                    wide[pl.ds(layer * heads + c * heads_per_chunk + h, sequences, stride=rows), :]
                    for h in range(heads_per_chunk)
                ],
                axis=1,
            ).astype(jnp.bfloat16)
            total += jnp.dot(
                lhs,
                weight_ref[layer, c * chunk : (c + 1) * chunk, :],
                preferred_element_type=jnp.float32,
            )
        low, high = total[:half], total[half:]
        mine_ref[layer] = jnp.where(first, low, high)
        other_ref[layer] = jnp.where(first, high, low)


def exchange(blocks):
    count = 2 * len(blocks)
    arrived = [blocks[0]]
    for k in range(1, len(blocks)):
        arrived.append(lax.ppermute(blocks[k], "seq", [(i, i ^ k) for i in range(count)]))
    return arrived


def params(limit):
    return pltpu.CompilerParams(vmem_limit_bytes=limit * MIB)


def in_hbm(*arrays):
    return [pltpu.with_memory_space_constraint(array, pltpu.HBM) for array in arrays]


def by_pairs(
    queries,
    new_keys,
    token_value_rows,
    cache_keys,
    prefill_value_cache,
    lengths,
    slot_index,
    out_proj,
):
    layers, _, heads, depth = queries.shape
    kv_heads = new_keys.shape[2]
    _, sequences, positions, _, _ = cache_keys.shape
    columns = out_proj.shape[2]
    pairs = sequences // 2
    bf16, f32 = jnp.bfloat16, jnp.float32
    flat = (layers, sequences, positions * kv_heads, depth)
    block = layers * positions * kv_heads
    query_rows, groups = layers * heads, layers * kv_heads
    side_rows = query_rows + 2 * groups
    block_shape = jax.ShapeDtypeStruct((2, 2, block, depth), bf16)
    *blocks, side = pl.pallas_call(
        functools.partial(stage_kernel, pairs),
        out_shape=[block_shape] * pairs + [jax.ShapeDtypeStruct((side_rows, depth), bf16)],
        in_specs=[HBM] * 6,
        out_specs=[VMEM] * (pairs + 1),
        scratch_shapes=[
            pltpu.SMEM((sequences,), jnp.int32),
            pltpu.VMEM(flat, bf16),
            pltpu.VMEM(flat, bf16),
            pltpu.SemaphoreType.DMA((6,)),
        ],
        compiler_params=params(4),
        cost_estimate=COVER,
    )(
        *in_hbm(
            slot_index,
            cache_keys.reshape(flat),
            prefill_value_cache.reshape(flat),
            queries.reshape(query_rows, depth),
            new_keys.reshape(groups, depth),
            token_value_rows.reshape(groups, depth),
        ),
    )
    blocks = exchange(blocks)
    limit = jnp.broadcast_to(lengths.astype(bf16)[:, None], (16, depth))
    packed = pl.pallas_call(
        pack_kernel,
        out_shape=jax.ShapeDtypeStruct((pairs * 4 * block + side_rows + 16, depth), bf16),
        in_specs=[VMEM] * (pairs + 2),
        out_specs=VMEM,
        compiler_params=params(4),
        cost_estimate=COVER,
    )(*blocks, side, limit)
    partner = lax.ppermute(packed, "seq", [(i, i ^ pairs) for i in range(sequences)])
    contexts = pl.pallas_call(
        functools.partial(pair_attend_kernel, pairs, layers, kv_heads, query_rows),
        out_shape=jax.ShapeDtypeStruct((2, query_rows, depth), bf16),
        in_specs=[VMEM] * (pairs + 3),
        out_specs=VMEM,
        compiler_params=params(4),
        cost_estimate=COVER,
    )(*blocks, side, limit, partner)
    contexts = exchange([contexts] * pairs)
    part = jax.ShapeDtypeStruct((layers, sequences // 2, columns), f32)
    mine, other = pl.pallas_call(
        functools.partial(pair_project_kernel, pairs, layers, 4 * depth),
        out_shape=(part, part),
        in_specs=[VMEM] * (pairs + 1),
        out_specs=(VMEM, VMEM),
        scratch_shapes=[pltpu.VMEM((sequences * query_rows, depth), f32)],
        compiler_params=params(24),
    )(*contexts, out_proj)
    arrived = lax.ppermute(other, "head", [(0, 1), (1, 0)])
    return (mine + arrived).astype(bf16)


def by_all_to_all(
    queries,
    new_keys,
    token_value_rows,
    cache_keys,
    prefill_value_cache,
    lengths,
    slot_index,
    out_proj,
):
    layers, _, heads, depth = queries.shape
    kv_heads = new_keys.shape[2]
    _, sequences, positions, _, _ = cache_keys.shape
    columns = out_proj.shape[2]
    bf16, f32 = jnp.bfloat16, jnp.float32
    flat = (layers, sequences, positions * kv_heads, depth)
    block = layers * positions * kv_heads
    picked = pl.pallas_call(
        pick_kernel,
        out_shape=jax.ShapeDtypeStruct((sequences, 2, block, depth), bf16),
        in_specs=[SMEM, ANY, ANY],
        out_specs=VMEM,
        scratch_shapes=[pltpu.SemaphoreType.DMA],
        compiler_params=pltpu.CompilerParams(vmem_limit_bytes=8 * 2**20),
    )(slot_index, cache_keys.reshape(flat), prefill_value_cache.reshape(flat))
    gathered = lax.all_to_all(picked, "seq", 0, 0, tiled=True)
    contexts = pl.pallas_call(
        functools.partial(attend_kernel, layers, kv_heads),
        out_shape=jax.ShapeDtypeStruct((sequences, layers * heads, depth), bf16),
        in_specs=[SMEM, VMEM, VMEM, VMEM, VMEM],
        out_specs=VMEM,
        compiler_params=pltpu.CompilerParams(vmem_limit_bytes=24 * 2**20),
    )(
        lengths,
        gathered,
        queries.reshape(layers * heads, depth),
        new_keys.reshape(layers * kv_heads, depth),
        token_value_rows.reshape(layers * kv_heads, depth),
    )
    contexts = lax.all_to_all(contexts, "seq", 0, 0, tiled=True)
    half = sequences // lax.axis_size("head")
    chunk = 4 * depth
    part = jax.ShapeDtypeStruct((layers, half, columns), f32)
    mine, other = pl.pallas_call(
        functools.partial(project_kernel, chunk),
        out_shape=(part, part),
        in_specs=[SMEM, VMEM, ANY],
        out_specs=(VMEM, VMEM),
        scratch_shapes=[
            pltpu.VMEM((sequences * layers * heads, depth), f32),
            pltpu.VMEM(out_proj.shape, bf16),
            pltpu.SemaphoreType.DMA((layers, heads * depth // chunk)),
        ],
        compiler_params=pltpu.CompilerParams(vmem_limit_bytes=40 * 2**20),
    )(lax.axis_index("head").reshape(1), contexts, out_proj)
    arrived = lax.ppermute(other, "head", [(0, 1), (1, 0)])
    return (mine + arrived).astype(bf16)


def solution(mesh):
    placed = (
        P(None, ("grp", "seq"), "head", None),
        P(None, ("grp", "seq"), "head", None),
        P(None, ("grp", "seq"), "head", None),
        P(None, "grp", "seq", "head", None),
        P(None, "grp", "seq", "head", None),
        P(("grp", "seq")),
        P("grp"),
        P(None, "head", "seq"),
    )
    seq = mesh.shape["seq"]
    few = seq in (2, 4, 8)

    def step(*operands):
        return (by_pairs if few else by_all_to_all)(*operands)

    step = jax.shard_map(
        step,
        mesh=mesh,
        in_specs=placed,
        out_specs=P(None, ("grp", "head"), "seq"),
        check_vma=False,
    )
    return step
```

```python
import functools

import jax
import jax.numpy as jnp
from jax import lax
from jax.experimental import pallas as pl
from jax.experimental.pallas import tpu as pltpu
from jax.sharding import PartitionSpec as P


VMEM = pl.BlockSpec(memory_space=pltpu.VMEM)
SMEM = pl.BlockSpec(memory_space=pltpu.SMEM)
ANY = pl.BlockSpec(memory_space=pl.ANY)
HBM = pl.BlockSpec(memory_space=pltpu.HBM)
MIB = 2**20
COVER = pl.CostEstimate(flops=10**10, bytes_accessed=2**20, transcendentals=0)


def pick_kernel(slot_ref, keys_ref, values_ref, out_ref, sem):
    layers, rows = keys_ref.shape[0], keys_ref.shape[2]

    @pl.loop(0, out_ref.shape[0], unroll=out_ref.shape[0] <= 8)
    def _(b):
        slot = slot_ref[b]
        for which, source in enumerate((keys_ref, values_ref)):
            for layer in range(layers):
                pltpu.make_async_copy(
                    source.at[layer, slot],
                    out_ref.at[b, which, pl.ds(layer * rows, rows), :],
                    sem,
                ).start()

    pltpu.make_async_copy(out_ref, out_ref, sem).wait()


def attend_kernel(layers, kv_heads, len_ref, kv_ref, q_ref, new_key_ref, new_value_ref, out_ref):
    sources, _, block, depth = kv_ref.shape
    groups = layers * kv_heads
    positions = block // groups
    queries = q_ref[...]
    keys = kv_ref[:, 0].reshape(sources * block, depth)
    values = kv_ref[:, 1].reshape(sources * block, depth)
    scaling = depth ** (-0.5)
    scores = lax.dot_general(
        queries, keys, (((1,), (1,)), ((), ())), preferred_element_type=jnp.float32
    )
    per_group = queries.shape[0] // groups
    shape = (groups, per_group, sources * block)
    scores = scores.reshape(shape) * scaling
    group = lax.broadcasted_iota(jnp.int32, shape, 0)
    column = lax.broadcasted_iota(jnp.int32, shape, 2)
    within = column % block
    column_group = (within // (positions * kv_heads)) * kv_heads + within % kv_heads
    position = (column // block) * positions + (within // kv_heads) % positions
    allowed = (column_group == group) & (position < len_ref[0])
    scores = jnp.where(allowed, scores, -1e30)
    grouped = queries.astype(jnp.float32).reshape(groups, per_group, depth)
    new_key = new_key_ref[...].astype(jnp.float32)[:, None, :]
    own_score = jnp.sum(grouped * new_key, axis=-1, keepdims=True) * scaling
    peak = jnp.maximum(jnp.max(scores, axis=-1, keepdims=True), own_score)
    raised = jnp.exp(scores - peak)
    own_raised = jnp.exp(own_score - peak)
    denominator = jnp.sum(raised, axis=-1, keepdims=True) + own_raised
    weights = (raised / denominator).astype(jnp.bfloat16)
    own_weight = (own_raised / denominator).astype(jnp.bfloat16)
    context = jnp.dot(
        weights.reshape(groups * per_group, sources * block),
        values,
        preferred_element_type=jnp.float32,
    ).reshape(groups, per_group, depth)
    new_value = new_value_ref[...].astype(jnp.float32)[:, None, :]
    context = context + own_weight.astype(jnp.float32) * new_value
    context = context.astype(jnp.bfloat16).reshape(groups * per_group, depth)
    out_ref[...] = jnp.broadcast_to(context[None], out_ref.shape)


def project_kernel(
    chunk, head_ref, context_ref, weight_ref, mine_ref, other_ref, wide, held, sems
):
    layers, depth_rows, columns = weight_ref.shape
    sequences, rows, depth = context_ref.shape
    heads = rows // layers
    chunks = depth_rows // chunk
    copies = []
    for layer in range(layers):
        for c in range(chunks):
            copies.append(
                pltpu.make_async_copy(
                    weight_ref.at[layer, pl.ds(c * chunk, chunk), :],
                    held.at[layer, pl.ds(c * chunk, chunk), :],
                    sems.at[layer, c],
                )
            )
            copies[-1].start()
    wide[...] = context_ref[...].astype(jnp.float32).reshape(sequences * rows, depth)
    heads_per_chunk = chunk // depth
    half = sequences // 2
    first = head_ref[0] == 0
    for layer in range(layers):
        total = jnp.zeros((sequences, columns), jnp.float32)
        for c in range(chunks):
            lhs = jnp.concatenate(
                [
                    wide[pl.ds(layer * heads + c * heads_per_chunk + h, sequences, stride=rows), :]
                    for h in range(heads_per_chunk)
                ],
                axis=1,
            ).astype(jnp.bfloat16)
            copies[layer * chunks + c].wait()
            total += jnp.dot(
                lhs,
                held[layer, c * chunk : (c + 1) * chunk, :],
                preferred_element_type=jnp.float32,
            )
        low, high = total[:half], total[half:]
        mine_ref[layer] = jnp.where(first, low, high)
        other_ref[layer] = jnp.where(first, high, low)


def softmax_context(queries, keys, values, allowed):
    _, depth = queries.shape
    scores = lax.dot_general(
        queries, keys, (((1,), (1,)), ((), ())), preferred_element_type=jnp.float32
    )
    scores = jnp.where(allowed, scores * depth ** (-0.5), -1e30)
    peak = jnp.max(scores, axis=-1, keepdims=True)
    raised = jnp.exp(scores - peak)
    denominator = jnp.sum(raised, axis=-1, keepdims=True)
    context = jnp.dot(raised.astype(jnp.bfloat16), values, preferred_element_type=jnp.float32)
    return (context / denominator).astype(jnp.bfloat16)


def place(pairs):
    index = lax.axis_index("seq")
    return index % pairs, index // pairs


def stage_kernel(
    pairs,
    slot_hbm,
    keys_hbm,
    values_hbm,
    queries_hbm,
    new_keys_hbm,
    new_values_hbm,
    *refs,
):
    blocks, side_ref = refs[:pairs], refs[pairs]
    slots, keys, values, sem = refs[pairs + 1 :]
    layers, _, rows, _ = keys.shape
    query_rows, new_rows = queries_hbm.shape[0], new_keys_hbm.shape[0]
    sources = (slot_hbm, keys_hbm, values_hbm, queries_hbm, new_keys_hbm, new_values_hbm)
    targets = (
        slots,
        keys,
        values,
        side_ref.at[pl.ds(0, query_rows)],
        side_ref.at[pl.ds(query_rows, new_rows)],
        side_ref.at[pl.ds(query_rows + new_rows, new_rows)],
    )
    copies = [
        pltpu.make_async_copy(source, target, sem.at[i])
        for i, (source, target) in enumerate(zip(sources, targets, strict=True))
    ]
    for copy in copies:
        copy.start()
    for copy in copies:
        copy.wait()
    pair, _ = place(pairs)
    for k in range(pairs):
        for side in range(2):
            slot = slots[side * pairs + (pair ^ k)]
            for which, held in enumerate((keys, values)):
                for layer in range(layers):
                    blocks[k][side, which, layer * rows : (layer + 1) * rows, :] = held[layer, slot]


def pack_kernel(*refs):
    start = 0
    for ref in refs[:-1]:
        rows = ref[...].reshape(-1, ref.shape[-1])
        refs[-1][start : start + rows.shape[0], :] = rows
        start += rows.shape[0]


def pair_attend_kernel(pairs, layers, kv_heads, query_rows, *refs):
    blocks, (side_ref, limit_ref, partner_ref, out_ref) = refs[:pairs], refs[pairs:]
    pair, mine = place(pairs)
    _, _, block, _ = blocks[0].shape
    groups = layers * kv_heads
    positions = block // groups
    per_block = 4 * block
    sources = 2 * pairs
    cached = sources * block
    shape = (query_rows, cached + groups)
    group = lax.broadcasted_iota(jnp.int32, shape, 0) // (query_rows // groups)
    column = lax.broadcasted_iota(jnp.int32, shape, 1)
    within = column % block
    column_group = (within // (positions * kv_heads)) * kv_heads + within % kv_heads
    source = column // block
    source = ((source // pairs) ^ mine) * pairs + ((source % pairs) ^ pair)
    position = source * positions + (within // kv_heads) % positions
    position = jnp.where(column < cached, position, -1).astype(jnp.float32)
    same_group = jnp.where(column < cached, column_group, column - cached) == group
    tail = pairs * per_block

    def side_rows(sequence, first, count):
        here = side_ref[first : first + count, :]
        there = partner_ref[tail + first : tail + first + count, :]
        return jnp.where(mine == sequence, here, there)

    for sequence in range(2):
        stacked = []
        for which in range(2):
            first = (sequence * 2 + which) * block
            stacked.append(
                jnp.concatenate(
                    [ref[sequence, which] for ref in blocks]
                    + [
                        partner_ref[k * per_block + first : k * per_block + first + block, :]
                        for k in range(pairs)
                    ]
                    + [side_rows(sequence, query_rows + which * groups, groups)],
                    axis=0,
                )
            )
        limit = jnp.where(
            mine == sequence, limit_ref[...], partner_ref[tail + query_rows + 2 * groups :, :]
        )
        allowed = same_group & (position < limit[:1, :1].astype(jnp.float32))
        out_ref[sequence] = softmax_context(
            side_rows(sequence, 0, query_rows), stacked[0], stacked[1], allowed
        )


def pair_project_kernel(pairs, layers, chunk, *refs):
    contexts, weight_ref, mine_ref, other_ref, wide = refs[:pairs], *refs[pairs:]
    _, rows, depth = contexts[0].shape
    heads = rows // layers
    sequences = 2 * pairs
    columns = weight_ref.shape[2]
    pair, _ = place(pairs)
    for k in range(pairs):
        for side in range(2):
            sequence = side * pairs + (pair ^ k)
            wide[pl.ds(pl.multiple_of(sequence * rows, rows), rows), :] = contexts[k][side].astype(
                jnp.float32
            )
    heads_per_chunk = chunk // depth
    half = sequences // 2
    first = lax.axis_index("head") == 0
    for layer in range(layers):
        total = jnp.zeros((sequences, columns), jnp.float32)
        for c in range(heads // heads_per_chunk):
            lhs = jnp.concatenate(
                [
                    wide[pl.ds(layer * heads + c * heads_per_chunk + h, sequences, stride=rows), :]
                    for h in range(heads_per_chunk)
                ],
                axis=1,
            ).astype(jnp.bfloat16)
            total += jnp.dot(
                lhs,
                weight_ref[layer, c * chunk : (c + 1) * chunk, :],
                preferred_element_type=jnp.float32,
            )
        low, high = total[:half], total[half:]
        mine_ref[layer] = jnp.where(first, low, high)
        other_ref[layer] = jnp.where(first, high, low)


def exchange(blocks):
    count = 2 * len(blocks)
    arrived = [blocks[0]]
    for k in range(1, len(blocks)):
        arrived.append(lax.ppermute(blocks[k], "seq", [(i, i ^ k) for i in range(count)]))
    return arrived


def params(limit):
    return pltpu.CompilerParams(vmem_limit_bytes=limit * MIB)


def in_hbm(*arrays):
    return [pltpu.with_memory_space_constraint(array, pltpu.HBM) for array in arrays]


def by_pairs(
    queries,
    new_keys,
    token_value_rows,
    cache_keys,
    prefill_value_cache,
    lengths,
    slot_index,
    out_proj,
):
    layers, _, heads, depth = queries.shape
    kv_heads = new_keys.shape[2]
    _, sequences, positions, _, _ = cache_keys.shape
    columns = out_proj.shape[2]
    pairs = sequences // 2
    bf16, f32 = jnp.bfloat16, jnp.float32
    flat = (layers, sequences, positions * kv_heads, depth)
    block = layers * positions * kv_heads
    query_rows, groups = layers * heads, layers * kv_heads
    side_rows = query_rows + 2 * groups
    block_shape = jax.ShapeDtypeStruct((2, 2, block, depth), bf16)
    *blocks, side = pl.pallas_call(
        functools.partial(stage_kernel, pairs),
        out_shape=[block_shape] * pairs + [jax.ShapeDtypeStruct((side_rows, depth), bf16)],
        in_specs=[HBM] * 6,
        out_specs=[VMEM] * (pairs + 1),
        scratch_shapes=[
            pltpu.SMEM((sequences,), jnp.int32),
            pltpu.VMEM(flat, bf16),
            pltpu.VMEM(flat, bf16),
            pltpu.SemaphoreType.DMA((6,)),
        ],
        compiler_params=params(4),
        cost_estimate=COVER,
    )(
        *in_hbm(
            slot_index,
            cache_keys.reshape(flat),
            prefill_value_cache.reshape(flat),
            queries.reshape(query_rows, depth),
            new_keys.reshape(groups, depth),
            token_value_rows.reshape(groups, depth),
        ),
    )
    blocks = exchange(blocks)
    limit = jnp.broadcast_to(lengths.astype(bf16)[:, None], (16, depth))
    packed = pl.pallas_call(
        pack_kernel,
        out_shape=jax.ShapeDtypeStruct((pairs * 4 * block + side_rows + 16, depth), bf16),
        in_specs=[VMEM] * (pairs + 2),
        out_specs=VMEM,
        compiler_params=params(4),
        cost_estimate=COVER,
    )(*blocks, side, limit)
    partner = lax.ppermute(packed, "seq", [(i, i ^ pairs) for i in range(sequences)])
    contexts = pl.pallas_call(
        functools.partial(pair_attend_kernel, pairs, layers, kv_heads, query_rows),
        out_shape=jax.ShapeDtypeStruct((2, query_rows, depth), bf16),
        in_specs=[VMEM] * (pairs + 3),
        out_specs=VMEM,
        compiler_params=params(4),
        cost_estimate=COVER,
    )(*blocks, side, limit, partner)
    contexts = exchange([contexts] * pairs)
    part = jax.ShapeDtypeStruct((layers, sequences // 2, columns), f32)
    mine, other = pl.pallas_call(
        functools.partial(pair_project_kernel, pairs, layers, 4 * depth),
        out_shape=(part, part),
        in_specs=[VMEM] * (pairs + 1),
        out_specs=(VMEM, VMEM),
        scratch_shapes=[pltpu.VMEM((sequences * query_rows, depth), f32)],
        compiler_params=params(24),
    )(*contexts, out_proj)
    arrived = lax.ppermute(other, "head", [(0, 1), (1, 0)])
    return (mine + arrived).astype(bf16)


def by_all_to_all(
    queries,
    new_keys,
    token_value_rows,
    cache_keys,
    prefill_value_cache,
    lengths,
    slot_index,
    out_proj,
):
    layers, _, heads, depth = queries.shape
    kv_heads = new_keys.shape[2]
    _, sequences, positions, _, _ = cache_keys.shape
    columns = out_proj.shape[2]
    bf16, f32 = jnp.bfloat16, jnp.float32
    flat = (layers, sequences, positions * kv_heads, depth)
    block = layers * positions * kv_heads
    picked = pl.pallas_call(
        pick_kernel,
        out_shape=jax.ShapeDtypeStruct((sequences, 2, block, depth), bf16),
        in_specs=[SMEM, ANY, ANY],
        out_specs=VMEM,
        scratch_shapes=[pltpu.SemaphoreType.DMA],
        compiler_params=pltpu.CompilerParams(vmem_limit_bytes=8 * 2**20),
    )(slot_index, cache_keys.reshape(flat), prefill_value_cache.reshape(flat))
    gathered = lax.all_to_all(picked, "seq", 0, 0, tiled=True)
    contexts = pl.pallas_call(
        functools.partial(attend_kernel, layers, kv_heads),
        out_shape=jax.ShapeDtypeStruct((sequences, layers * heads, depth), bf16),
        in_specs=[SMEM, VMEM, VMEM, VMEM, VMEM],
        out_specs=VMEM,
        compiler_params=pltpu.CompilerParams(vmem_limit_bytes=24 * 2**20),
    )(
        lengths,
        gathered,
        queries.reshape(layers * heads, depth),
        new_keys.reshape(layers * kv_heads, depth),
        token_value_rows.reshape(layers * kv_heads, depth),
    )
    contexts = lax.all_to_all(contexts, "seq", 0, 0, tiled=True)
    half = sequences // lax.axis_size("head")
    chunk = 4 * depth
    part = jax.ShapeDtypeStruct((layers, half, columns), f32)
    mine, other = pl.pallas_call(
        functools.partial(project_kernel, chunk),
        out_shape=(part, part),
        in_specs=[SMEM, VMEM, ANY],
        out_specs=(VMEM, VMEM),
        scratch_shapes=[
            pltpu.VMEM((sequences * layers * heads, depth), f32),
            pltpu.VMEM(out_proj.shape, bf16),
            pltpu.SemaphoreType.DMA((layers, heads * depth // chunk)),
        ],
        compiler_params=pltpu.CompilerParams(vmem_limit_bytes=40 * 2**20),
    )(lax.axis_index("head").reshape(1), contexts, out_proj)
    arrived = lax.ppermute(other, "head", [(0, 1), (1, 0)])
    return (mine + arrived).astype(bf16)


def solution(mesh):
    placed = (
        P(None, ("grp", "seq"), "head", None),
        P(None, ("grp", "seq"), "head", None),
        P(None, ("grp", "seq"), "head", None),
        P(None, "grp", "seq", "head", None),
        P(None, "grp", "seq", "head", None),
        P(("grp", "seq")),
        P("grp"),
        P(None, "head", "seq"),
    )
    seq = mesh.shape["seq"]
    few = seq in (2, 4, 8)

    def step(*operands):
        return (by_pairs if few else by_all_to_all)(*operands)

    step = jax.shard_map(
        step,
        mesh=mesh,
        in_specs=placed,
        out_specs=P(None, ("grp", "head"), "seq"),
        check_vma=False,
    )
    return step
```

```python
import functools

import jax
import jax.numpy as jnp
from jax import lax
from jax.experimental import pallas as pl
from jax.experimental.pallas import tpu as pltpu
from jax.sharding import PartitionSpec as P


VMEM = pl.BlockSpec(memory_space=pltpu.VMEM)
SMEM = pl.BlockSpec(memory_space=pltpu.SMEM)
ANY = pl.BlockSpec(memory_space=pl.ANY)
HBM = pl.BlockSpec(memory_space=pltpu.HBM)
MIB = 2**20
COVER = pl.CostEstimate(flops=10**10, bytes_accessed=2**20, transcendentals=0)


def pick_kernel(slot_ref, keys_ref, values_ref, out_ref, sem):
    layers, rows = keys_ref.shape[0], keys_ref.shape[2]

    @pl.loop(0, out_ref.shape[0], unroll=out_ref.shape[0] <= 8)
    def _(b):
        slot = slot_ref[b]
        for which, source in enumerate((keys_ref, values_ref)):
            for layer in range(layers):
                pltpu.make_async_copy(
                    source.at[layer, slot],
                    out_ref.at[b, which, pl.ds(layer * rows, rows), :],
                    sem,
                ).start()

    pltpu.make_async_copy(out_ref, out_ref, sem).wait()


def attend_kernel(layers, kv_heads, len_ref, kv_ref, q_ref, new_key_ref, new_value_ref, out_ref):
    sources, _, block, depth = kv_ref.shape
    groups = layers * kv_heads
    positions = block // groups
    queries = q_ref[...]
    keys = kv_ref[:, 0].reshape(sources * block, depth)
    values = kv_ref[:, 1].reshape(sources * block, depth)
    scaling = depth ** (-0.5)
    scores = lax.dot_general(
        queries, keys, (((1,), (1,)), ((), ())), preferred_element_type=jnp.float32
    )
    per_group = queries.shape[0] // groups
    shape = (groups, per_group, sources * block)
    scores = scores.reshape(shape) * scaling
    group = lax.broadcasted_iota(jnp.int32, shape, 0)
    column = lax.broadcasted_iota(jnp.int32, shape, 2)
    within = column % block
    column_group = (within // (positions * kv_heads)) * kv_heads + within % kv_heads
    position = (column // block) * positions + (within // kv_heads) % positions
    allowed = (column_group == group) & (position < len_ref[0])
    scores = jnp.where(allowed, scores, -1e30)
    grouped = queries.astype(jnp.float32).reshape(groups, per_group, depth)
    new_key = new_key_ref[...].astype(jnp.float32)[:, None, :]
    own_score = jnp.sum(grouped * new_key, axis=-1, keepdims=True) * scaling
    peak = jnp.maximum(jnp.max(scores, axis=-1, keepdims=True), own_score)
    raised = jnp.exp(scores - peak)
    own_raised = jnp.exp(own_score - peak)
    denominator = jnp.sum(raised, axis=-1, keepdims=True) + own_raised
    weights = (raised / denominator).astype(jnp.bfloat16)
    own_weight = (own_raised / denominator).astype(jnp.bfloat16)
    context = jnp.dot(
        weights.reshape(groups * per_group, sources * block),
        values,
        preferred_element_type=jnp.float32,
    ).reshape(groups, per_group, depth)
    new_value = new_value_ref[...].astype(jnp.float32)[:, None, :]
    context = context + own_weight.astype(jnp.float32) * new_value
    context = context.astype(jnp.bfloat16).reshape(groups * per_group, depth)
    out_ref[...] = jnp.broadcast_to(context[None], out_ref.shape)


def project_kernel(
    chunk, head_ref, context_ref, weight_ref, mine_ref, other_ref, wide, held, sems
):
    layers, depth_rows, columns = weight_ref.shape
    sequences, rows, depth = context_ref.shape
    heads = rows // layers
    chunks = depth_rows // chunk
    copies = []
    for layer in range(layers):
        for c in range(chunks):
            copies.append(
                pltpu.make_async_copy(
                    weight_ref.at[layer, pl.ds(c * chunk, chunk), :],
                    held.at[layer, pl.ds(c * chunk, chunk), :],
                    sems.at[layer, c],
                )
            )
            copies[-1].start()
    wide[...] = context_ref[...].astype(jnp.float32).reshape(sequences * rows, depth)
    heads_per_chunk = chunk // depth
    half = sequences // 2
    first = head_ref[0] == 0
    for layer in range(layers):
        total = jnp.zeros((sequences, columns), jnp.float32)
        for c in range(chunks):
            lhs = jnp.concatenate(
                [
                    wide[pl.ds(layer * heads + c * heads_per_chunk + h, sequences, stride=rows), :]
                    for h in range(heads_per_chunk)
                ],
                axis=1,
            ).astype(jnp.bfloat16)
            copies[layer * chunks + c].wait()
            total += jnp.dot(
                lhs,
                held[layer, c * chunk : (c + 1) * chunk, :],
                preferred_element_type=jnp.float32,
            )
        low, high = total[:half], total[half:]
        mine_ref[layer] = jnp.where(first, low, high)
        other_ref[layer] = jnp.where(first, high, low)


def softmax_context(queries, keys, values, allowed):
    _, depth = queries.shape
    scores = lax.dot_general(
        queries, keys, (((1,), (1,)), ((), ())), preferred_element_type=jnp.float32
    )
    scores = jnp.where(allowed, scores * depth ** (-0.5), -1e30)
    peak = jnp.max(scores, axis=-1, keepdims=True)
    raised = jnp.exp(scores - peak)
    denominator = jnp.sum(raised, axis=-1, keepdims=True)
    context = jnp.dot(raised.astype(jnp.bfloat16), values, preferred_element_type=jnp.float32)
    return (context / denominator).astype(jnp.bfloat16)


def place(pairs):
    index = lax.axis_index("seq")
    return index % pairs, index // pairs


def stage_kernel(pairs, slot_hbm, keys_hbm, values_hbm, *refs):
    blocks, (slots, keys, values, sem) = refs[:pairs], refs[pairs:]
    layers, _, rows, _ = keys.shape
    targets = (slots, keys, values)
    copies = [
        pltpu.make_async_copy(source, target, sem.at[i])
        for i, (source, target) in enumerate(
            zip((slot_hbm, keys_hbm, values_hbm), targets, strict=True)
        )
    ]
    for copy in copies:
        copy.start()
    for copy in copies:
        copy.wait()
    pair, _ = place(pairs)
    for k in range(pairs):
        for side in range(2):
            slot = slots[side * pairs + (pair ^ k)]
            for which, held in enumerate((keys, values)):
                for layer in range(layers):
                    blocks[k][side, which, layer * rows : (layer + 1) * rows, :] = held[layer, slot]


def own_rows_kernel(queries_hbm, new_keys_hbm, new_values_hbm, side_ref, sem):
    copies = []
    start = 0
    for i, source in enumerate((queries_hbm, new_keys_hbm, new_values_hbm)):
        target = side_ref.at[pl.ds(start, source.shape[0])]
        copies.append(pltpu.make_async_copy(source, target, sem.at[i]))
        copies[-1].start()
        start += source.shape[0]
    for copy in copies:
        copy.wait()


def pack_kernel(*refs):
    start = 0
    for ref in refs[:-1]:
        rows = ref[...].reshape(-1, ref.shape[-1])
        refs[-1][start : start + rows.shape[0], :] = rows
        start += rows.shape[0]


def pair_attend_kernel(pairs, layers, kv_heads, query_rows, *refs):
    blocks, (side_ref, limit_ref, partner_ref, out_ref) = refs[:pairs], refs[pairs:]
    pair, mine = place(pairs)
    _, _, block, _ = blocks[0].shape
    groups = layers * kv_heads
    positions = block // groups
    per_block = 4 * block
    sources = 2 * pairs
    cached = sources * block
    shape = (query_rows, cached + groups)
    group = lax.broadcasted_iota(jnp.int32, shape, 0) // (query_rows // groups)
    column = lax.broadcasted_iota(jnp.int32, shape, 1)
    within = column % block
    column_group = (within // (positions * kv_heads)) * kv_heads + within % kv_heads
    source = column // block
    source = ((source // pairs) ^ mine) * pairs + ((source % pairs) ^ pair)
    position = source * positions + (within // kv_heads) % positions
    position = jnp.where(column < cached, position, -1).astype(jnp.float32)
    same_group = jnp.where(column < cached, column_group, column - cached) == group
    tail = pairs * per_block

    def side_rows(sequence, first, count):
        here = side_ref[first : first + count, :]
        there = partner_ref[tail + first : tail + first + count, :]
        return jnp.where(mine == sequence, here, there)

    for sequence in range(2):
        stacked = []
        for which in range(2):
            first = (sequence * 2 + which) * block
            stacked.append(
                jnp.concatenate(
                    [ref[sequence, which] for ref in blocks]
                    + [
                        partner_ref[k * per_block + first : k * per_block + first + block, :]
                        for k in range(pairs)
                    ]
                    + [side_rows(sequence, query_rows + which * groups, groups)],
                    axis=0,
                )
            )
        limit = jnp.where(
            mine == sequence, limit_ref[...], partner_ref[tail + query_rows + 2 * groups :, :]
        )
        allowed = same_group & (position < limit[:1, :1].astype(jnp.float32))
        out_ref[sequence] = softmax_context(
            side_rows(sequence, 0, query_rows), stacked[0], stacked[1], allowed
        )


def pair_project_kernel(pairs, layers, chunk, *refs):
    contexts, weight_ref, mine_ref, other_ref, wide = refs[:pairs], *refs[pairs:]
    _, rows, depth = contexts[0].shape
    heads = rows // layers
    sequences = 2 * pairs
    columns = weight_ref.shape[2]
    pair, _ = place(pairs)
    for k in range(pairs):
        for side in range(2):
            sequence = side * pairs + (pair ^ k)
            wide[pl.ds(pl.multiple_of(sequence * rows, rows), rows), :] = contexts[k][side].astype(
                jnp.float32
            )
    heads_per_chunk = chunk // depth
    half = sequences // 2
    first = lax.axis_index("head") == 0
    for layer in range(layers):
        total = jnp.zeros((sequences, columns), jnp.float32)
        for c in range(heads // heads_per_chunk):
            lhs = jnp.concatenate(
                [
                    wide[pl.ds(layer * heads + c * heads_per_chunk + h, sequences, stride=rows), :]
                    for h in range(heads_per_chunk)
                ],
                axis=1,
            ).astype(jnp.bfloat16)
            total += jnp.dot(
                lhs,
                weight_ref[layer, c * chunk : (c + 1) * chunk, :],
                preferred_element_type=jnp.float32,
            )
        low, high = total[:half], total[half:]
        mine_ref[layer] = jnp.where(first, low, high)
        other_ref[layer] = jnp.where(first, high, low)


def exchange(blocks):
    count = 2 * len(blocks)
    arrived = [blocks[0]]
    for k in range(1, len(blocks)):
        arrived.append(lax.ppermute(blocks[k], "seq", [(i, i ^ k) for i in range(count)]))
    return arrived


def params(limit):
    return pltpu.CompilerParams(vmem_limit_bytes=limit * MIB)


def in_hbm(*arrays):
    return [pltpu.with_memory_space_constraint(array, pltpu.HBM) for array in arrays]


def by_pairs(
    queries,
    new_keys,
    token_value_rows,
    cache_keys,
    prefill_value_cache,
    lengths,
    slot_index,
    out_proj,
):
    layers, _, heads, depth = queries.shape
    kv_heads = new_keys.shape[2]
    _, sequences, positions, _, _ = cache_keys.shape
    columns = out_proj.shape[2]
    pairs = sequences // 2
    bf16, f32 = jnp.bfloat16, jnp.float32
    flat = (layers, sequences, positions * kv_heads, depth)
    block = layers * positions * kv_heads
    query_rows, groups = layers * heads, layers * kv_heads
    side_rows = query_rows + 2 * groups
    block_shape = jax.ShapeDtypeStruct((2, 2, block, depth), bf16)
    blocks = pl.pallas_call(
        functools.partial(stage_kernel, pairs),
        out_shape=[block_shape] * pairs,
        in_specs=[HBM] * 3,
        out_specs=[VMEM] * pairs,
        scratch_shapes=[
            pltpu.SMEM((sequences,), jnp.int32),
            pltpu.VMEM(flat, bf16),
            pltpu.VMEM(flat, bf16),
            pltpu.SemaphoreType.DMA((3,)),
        ],
        compiler_params=params(4),
        cost_estimate=COVER,
    )(
        *in_hbm(slot_index, cache_keys.reshape(flat), prefill_value_cache.reshape(flat)),
    )
    blocks = exchange(blocks)
    side = pl.pallas_call(
        own_rows_kernel,
        out_shape=jax.ShapeDtypeStruct((side_rows, depth), bf16),
        in_specs=[HBM] * 3,
        out_specs=VMEM,
        scratch_shapes=[pltpu.SemaphoreType.DMA((3,))],
        compiler_params=params(4),
        cost_estimate=COVER,
    )(
        *in_hbm(
            queries.reshape(query_rows, depth),
            new_keys.reshape(groups, depth),
            token_value_rows.reshape(groups, depth),
        ),
    )
    limit = jnp.broadcast_to(lengths.astype(bf16)[:, None], (8, depth))
    packed = pl.pallas_call(
        pack_kernel,
        out_shape=jax.ShapeDtypeStruct((pairs * 4 * block + side_rows + 8, depth), bf16),
        in_specs=[VMEM] * (pairs + 2),
        out_specs=VMEM,
        compiler_params=params(4),
        cost_estimate=COVER,
    )(*blocks, side, limit)
    partner = lax.ppermute(packed, "seq", [(i, i ^ pairs) for i in range(sequences)])
    contexts = pl.pallas_call(
        functools.partial(pair_attend_kernel, pairs, layers, kv_heads, query_rows),
        out_shape=jax.ShapeDtypeStruct((2, query_rows, depth), bf16),
        in_specs=[VMEM] * (pairs + 3),
        out_specs=VMEM,
        compiler_params=params(4),
        cost_estimate=COVER,
    )(*blocks, side, limit, partner)
    contexts = exchange([contexts] * pairs)
    part = jax.ShapeDtypeStruct((layers, sequences // 2, columns), f32)
    mine, other = pl.pallas_call(
        functools.partial(pair_project_kernel, pairs, layers, 4 * depth),
        out_shape=(part, part),
        in_specs=[VMEM] * (pairs + 1),
        out_specs=(VMEM, VMEM),
        scratch_shapes=[pltpu.VMEM((sequences * query_rows, depth), f32)],
        compiler_params=params(24),
    )(*contexts, out_proj)
    arrived = lax.ppermute(other, "head", [(0, 1), (1, 0)])
    return (mine + arrived).astype(bf16)


def by_all_to_all(
    queries,
    new_keys,
    token_value_rows,
    cache_keys,
    prefill_value_cache,
    lengths,
    slot_index,
    out_proj,
):
    layers, _, heads, depth = queries.shape
    kv_heads = new_keys.shape[2]
    _, sequences, positions, _, _ = cache_keys.shape
    columns = out_proj.shape[2]
    bf16, f32 = jnp.bfloat16, jnp.float32
    flat = (layers, sequences, positions * kv_heads, depth)
    block = layers * positions * kv_heads
    picked = pl.pallas_call(
        pick_kernel,
        out_shape=jax.ShapeDtypeStruct((sequences, 2, block, depth), bf16),
        in_specs=[SMEM, ANY, ANY],
        out_specs=VMEM,
        scratch_shapes=[pltpu.SemaphoreType.DMA],
        compiler_params=pltpu.CompilerParams(vmem_limit_bytes=8 * 2**20),
    )(slot_index, cache_keys.reshape(flat), prefill_value_cache.reshape(flat))
    gathered = lax.all_to_all(picked, "seq", 0, 0, tiled=True)
    contexts = pl.pallas_call(
        functools.partial(attend_kernel, layers, kv_heads),
        out_shape=jax.ShapeDtypeStruct((sequences, layers * heads, depth), bf16),
        in_specs=[SMEM, VMEM, VMEM, VMEM, VMEM],
        out_specs=VMEM,
        compiler_params=pltpu.CompilerParams(vmem_limit_bytes=24 * 2**20),
    )(
        lengths,
        gathered,
        queries.reshape(layers * heads, depth),
        new_keys.reshape(layers * kv_heads, depth),
        token_value_rows.reshape(layers * kv_heads, depth),
    )
    contexts = lax.all_to_all(contexts, "seq", 0, 0, tiled=True)
    half = sequences // lax.axis_size("head")
    chunk = 4 * depth
    part = jax.ShapeDtypeStruct((layers, half, columns), f32)
    mine, other = pl.pallas_call(
        functools.partial(project_kernel, chunk),
        out_shape=(part, part),
        in_specs=[SMEM, VMEM, ANY],
        out_specs=(VMEM, VMEM),
        scratch_shapes=[
            pltpu.VMEM((sequences * layers * heads, depth), f32),
            pltpu.VMEM(out_proj.shape, bf16),
            pltpu.SemaphoreType.DMA((layers, heads * depth // chunk)),
        ],
        compiler_params=pltpu.CompilerParams(vmem_limit_bytes=40 * 2**20),
    )(lax.axis_index("head").reshape(1), contexts, out_proj)
    arrived = lax.ppermute(other, "head", [(0, 1), (1, 0)])
    return (mine + arrived).astype(bf16)


def solution(mesh):
    placed = (
        P(None, ("grp", "seq"), "head", None),
        P(None, ("grp", "seq"), "head", None),
        P(None, ("grp", "seq"), "head", None),
        P(None, "grp", "seq", "head", None),
        P(None, "grp", "seq", "head", None),
        P(("grp", "seq")),
        P("grp"),
        P(None, "head", "seq"),
    )
    seq = mesh.shape["seq"]
    few = seq in (2, 4, 8)

    def step(*operands):
        return (by_pairs if few else by_all_to_all)(*operands)

    step = jax.shard_map(
        step,
        mesh=mesh,
        in_specs=placed,
        out_specs=P(None, ("grp", "head"), "seq"),
        check_vma=False,
    )
    return step
```

```python
import functools

import jax
import jax.numpy as jnp
from jax import lax
from jax.experimental import pallas as pl
from jax.experimental.pallas import tpu as pltpu
from jax.sharding import PartitionSpec as P


VMEM = pl.BlockSpec(memory_space=pltpu.VMEM)
SMEM = pl.BlockSpec(memory_space=pltpu.SMEM)
ANY = pl.BlockSpec(memory_space=pl.ANY)
HBM = pl.BlockSpec(memory_space=pltpu.HBM)
MIB = 2**20
COVER = pl.CostEstimate(flops=10**10, bytes_accessed=2**20, transcendentals=0)


def pick_kernel(slot_ref, keys_ref, values_ref, out_ref, sem):
    layers, rows = keys_ref.shape[0], keys_ref.shape[2]

    @pl.loop(0, out_ref.shape[0], unroll=out_ref.shape[0] <= 8)
    def _(b):
        slot = slot_ref[b]
        for which, source in enumerate((keys_ref, values_ref)):
            for layer in range(layers):
                pltpu.make_async_copy(
                    source.at[layer, slot],
                    out_ref.at[b, which, pl.ds(layer * rows, rows), :],
                    sem,
                ).start()

    pltpu.make_async_copy(out_ref, out_ref, sem).wait()


def attend_kernel(layers, kv_heads, len_ref, kv_ref, q_ref, new_key_ref, new_value_ref, out_ref):
    sources, _, block, depth = kv_ref.shape
    groups = layers * kv_heads
    positions = block // groups
    queries = q_ref[...]
    keys = kv_ref[:, 0].reshape(sources * block, depth)
    values = kv_ref[:, 1].reshape(sources * block, depth)
    scaling = depth ** (-0.5)
    scores = lax.dot_general(
        queries, keys, (((1,), (1,)), ((), ())), preferred_element_type=jnp.float32
    )
    per_group = queries.shape[0] // groups
    shape = (groups, per_group, sources * block)
    scores = scores.reshape(shape) * scaling
    group = lax.broadcasted_iota(jnp.int32, shape, 0)
    column = lax.broadcasted_iota(jnp.int32, shape, 2)
    within = column % block
    column_group = (within // (positions * kv_heads)) * kv_heads + within % kv_heads
    position = (column // block) * positions + (within // kv_heads) % positions
    allowed = (column_group == group) & (position < len_ref[0])
    scores = jnp.where(allowed, scores, -1e30)
    grouped = queries.astype(jnp.float32).reshape(groups, per_group, depth)
    new_key = new_key_ref[...].astype(jnp.float32)[:, None, :]
    own_score = jnp.sum(grouped * new_key, axis=-1, keepdims=True) * scaling
    peak = jnp.maximum(jnp.max(scores, axis=-1, keepdims=True), own_score)
    raised = jnp.exp(scores - peak)
    own_raised = jnp.exp(own_score - peak)
    denominator = jnp.sum(raised, axis=-1, keepdims=True) + own_raised
    weights = (raised / denominator).astype(jnp.bfloat16)
    own_weight = (own_raised / denominator).astype(jnp.bfloat16)
    context = jnp.dot(
        weights.reshape(groups * per_group, sources * block),
        values,
        preferred_element_type=jnp.float32,
    ).reshape(groups, per_group, depth)
    new_value = new_value_ref[...].astype(jnp.float32)[:, None, :]
    context = context + own_weight.astype(jnp.float32) * new_value
    context = context.astype(jnp.bfloat16).reshape(groups * per_group, depth)
    out_ref[...] = jnp.broadcast_to(context[None], out_ref.shape)


def project_kernel(
    chunk, head_ref, context_ref, weight_ref, mine_ref, other_ref, wide, held, sems
):
    layers, depth_rows, columns = weight_ref.shape
    sequences, rows, depth = context_ref.shape
    heads = rows // layers
    chunks = depth_rows // chunk
    copies = []
    for layer in range(layers):
        for c in range(chunks):
            copies.append(
                pltpu.make_async_copy(
                    weight_ref.at[layer, pl.ds(c * chunk, chunk), :],
                    held.at[layer, pl.ds(c * chunk, chunk), :],
                    sems.at[layer, c],
                )
            )
            copies[-1].start()
    wide[...] = context_ref[...].astype(jnp.float32).reshape(sequences * rows, depth)
    heads_per_chunk = chunk // depth
    half = sequences // 2
    first = head_ref[0] == 0
    for layer in range(layers):
        total = jnp.zeros((sequences, columns), jnp.float32)
        for c in range(chunks):
            lhs = jnp.concatenate(
                [
                    wide[pl.ds(layer * heads + c * heads_per_chunk + h, sequences, stride=rows), :]
                    for h in range(heads_per_chunk)
                ],
                axis=1,
            ).astype(jnp.bfloat16)
            copies[layer * chunks + c].wait()
            total += jnp.dot(
                lhs,
                held[layer, c * chunk : (c + 1) * chunk, :],
                preferred_element_type=jnp.float32,
            )
        low, high = total[:half], total[half:]
        mine_ref[layer] = jnp.where(first, low, high)
        other_ref[layer] = jnp.where(first, high, low)


def softmax_context(queries, keys, values, allowed):
    _, depth = queries.shape
    scores = lax.dot_general(
        queries, keys, (((1,), (1,)), ((), ())), preferred_element_type=jnp.float32
    )
    scores = jnp.where(allowed, scores * depth ** (-0.5), -1e30)
    peak = jnp.max(scores, axis=-1, keepdims=True)
    raised = jnp.exp(scores - peak)
    denominator = jnp.sum(raised, axis=-1, keepdims=True)
    context = jnp.dot(raised.astype(jnp.bfloat16), values, preferred_element_type=jnp.float32)
    return (context / denominator).astype(jnp.bfloat16)


def place(pairs):
    index = lax.axis_index("seq")
    return index % pairs, index // pairs


def stage_kernel(pairs, slot_hbm, keys_hbm, values_hbm, *refs):
    blocks, (slots, keys, values, sem) = refs[:pairs], refs[pairs:]
    layers, _, rows, _ = keys.shape
    targets = (slots, keys, values)
    copies = [
        pltpu.make_async_copy(source, target, sem.at[i])
        for i, (source, target) in enumerate(
            zip((slot_hbm, keys_hbm, values_hbm), targets, strict=True)
        )
    ]
    for copy in copies:
        copy.start()
    for copy in copies:
        copy.wait()
    pair, _ = place(pairs)
    for k in range(pairs):
        for side in range(2):
            slot = slots[side * pairs + (pair ^ k)]
            for which, held in enumerate((keys, values)):
                for layer in range(layers):
                    blocks[k][side, which, layer * rows : (layer + 1) * rows, :] = held[layer, slot]


def own_rows_kernel(queries_hbm, new_keys_hbm, new_values_hbm, side_ref, sem):
    copies = []
    start = 0
    for i, source in enumerate((queries_hbm, new_keys_hbm, new_values_hbm)):
        target = side_ref.at[pl.ds(start, source.shape[0])]
        copies.append(pltpu.make_async_copy(source, target, sem.at[i]))
        copies[-1].start()
        start += source.shape[0]
    for copy in copies:
        copy.wait()


def pack_kernel(*refs):
    start = 0
    for ref in refs[:-1]:
        rows = ref[...].reshape(-1, ref.shape[-1])
        refs[-1][start : start + rows.shape[0], :] = rows
        start += rows.shape[0]


def pair_attend_kernel(pairs, layers, kv_heads, query_rows, *refs):
    blocks, (side_ref, limit_ref, partner_ref, out_ref) = refs[:pairs], refs[pairs:]
    pair, mine = place(pairs)
    _, _, block, _ = blocks[0].shape
    groups = layers * kv_heads
    positions = block // groups
    per_block = 4 * block
    sources = 2 * pairs
    cached = sources * block
    group = lax.broadcasted_iota(jnp.int32, (query_rows, 1), 0) // (query_rows // groups)
    column = lax.broadcasted_iota(jnp.int32, (1, cached + groups), 1)
    within = column % block
    column_group = (within // (positions * kv_heads)) * kv_heads + within % kv_heads
    source = column // block
    source = ((source // pairs) ^ mine) * pairs + ((source % pairs) ^ pair)
    position = source * positions + (within // kv_heads) % positions
    position = jnp.where(column < cached, position, -1).astype(jnp.float32)
    same_group = jnp.where(column < cached, column_group, column - cached) == group
    tail = pairs * per_block

    def side_rows(sequence, first, count):
        here = side_ref[first : first + count, :]
        there = partner_ref[tail + first : tail + first + count, :]
        return jnp.where(mine == sequence, here, there)

    for sequence in range(2):
        stacked = []
        for which in range(2):
            first = (sequence * 2 + which) * block
            stacked.append(
                jnp.concatenate(
                    [ref[sequence, which] for ref in blocks]
                    + [
                        partner_ref[k * per_block + first : k * per_block + first + block, :]
                        for k in range(pairs)
                    ]
                    + [side_rows(sequence, query_rows + which * groups, groups)],
                    axis=0,
                )
            )
        limit = jnp.where(
            mine == sequence, limit_ref[...], partner_ref[tail + query_rows + 2 * groups :, :]
        )
        allowed = same_group & (position < limit[:1, :1].astype(jnp.float32))
        out_ref[sequence] = softmax_context(
            side_rows(sequence, 0, query_rows), stacked[0], stacked[1], allowed
        )


def pair_project_kernel(pairs, layers, chunk, *refs):
    contexts, weight_ref, mine_ref, other_ref, wide = refs[:pairs], *refs[pairs:]
    _, rows, depth = contexts[0].shape
    heads = rows // layers
    sequences = 2 * pairs
    columns = weight_ref.shape[2]
    pair, _ = place(pairs)
    for k in range(pairs):
        for side in range(2):
            sequence = side * pairs + (pair ^ k)
            wide[pl.ds(pl.multiple_of(sequence * rows, rows), rows), :] = contexts[k][side].astype(
                jnp.float32
            )
    heads_per_chunk = chunk // depth
    half = sequences // 2
    first = lax.axis_index("head") == 0
    for layer in range(layers):
        total = jnp.zeros((sequences, columns), jnp.float32)
        for c in range(heads // heads_per_chunk):
            lhs = jnp.concatenate(
                [
                    wide[pl.ds(layer * heads + c * heads_per_chunk + h, sequences, stride=rows), :]
                    for h in range(heads_per_chunk)
                ],
                axis=1,
            ).astype(jnp.bfloat16)
            total += jnp.dot(
                lhs,
                weight_ref[layer, c * chunk : (c + 1) * chunk, :],
                preferred_element_type=jnp.float32,
            )
        low, high = total[:half], total[half:]
        mine_ref[layer] = jnp.where(first, low, high)
        other_ref[layer] = jnp.where(first, high, low)


def exchange(blocks):
    count = 2 * len(blocks)
    arrived = [blocks[0]]
    for k in range(1, len(blocks)):
        arrived.append(lax.ppermute(blocks[k], "seq", [(i, i ^ k) for i in range(count)]))
    return arrived


def params(limit):
    return pltpu.CompilerParams(vmem_limit_bytes=limit * MIB)


def in_hbm(*arrays):
    return [pltpu.with_memory_space_constraint(array, pltpu.HBM) for array in arrays]


def by_pairs(
    queries,
    new_keys,
    token_value_rows,
    cache_keys,
    prefill_value_cache,
    lengths,
    slot_index,
    out_proj,
):
    layers, _, heads, depth = queries.shape
    kv_heads = new_keys.shape[2]
    _, sequences, positions, _, _ = cache_keys.shape
    columns = out_proj.shape[2]
    pairs = sequences // 2
    bf16, f32 = jnp.bfloat16, jnp.float32
    flat = (layers, sequences, positions * kv_heads, depth)
    block = layers * positions * kv_heads
    query_rows, groups = layers * heads, layers * kv_heads
    side_rows = query_rows + 2 * groups
    block_shape = jax.ShapeDtypeStruct((2, 2, block, depth), bf16)
    blocks = pl.pallas_call(
        functools.partial(stage_kernel, pairs),
        out_shape=[block_shape] * pairs,
        in_specs=[HBM] * 3,
        out_specs=[VMEM] * pairs,
        scratch_shapes=[
            pltpu.SMEM((sequences,), jnp.int32),
            pltpu.VMEM(flat, bf16),
            pltpu.VMEM(flat, bf16),
            pltpu.SemaphoreType.DMA((3,)),
        ],
        compiler_params=params(4),
        cost_estimate=COVER,
    )(
        *in_hbm(slot_index, cache_keys.reshape(flat), prefill_value_cache.reshape(flat)),
    )
    blocks = exchange(blocks)
    side = pl.pallas_call(
        own_rows_kernel,
        out_shape=jax.ShapeDtypeStruct((side_rows, depth), bf16),
        in_specs=[HBM] * 3,
        out_specs=VMEM,
        scratch_shapes=[pltpu.SemaphoreType.DMA((3,))],
        compiler_params=params(4),
        cost_estimate=COVER,
    )(
        *in_hbm(
            queries.reshape(query_rows, depth),
            new_keys.reshape(groups, depth),
            token_value_rows.reshape(groups, depth),
        ),
    )
    limit = jnp.broadcast_to(lengths.astype(bf16)[:, None], (8, depth))
    packed = pl.pallas_call(
        pack_kernel,
        out_shape=jax.ShapeDtypeStruct((pairs * 4 * block + side_rows + 8, depth), bf16),
        in_specs=[VMEM] * (pairs + 2),
        out_specs=VMEM,
        compiler_params=params(4),
        cost_estimate=COVER,
    )(*blocks, side, limit)
    partner = lax.ppermute(packed, "seq", [(i, i ^ pairs) for i in range(sequences)])
    contexts = pl.pallas_call(
        functools.partial(pair_attend_kernel, pairs, layers, kv_heads, query_rows),
        out_shape=jax.ShapeDtypeStruct((2, query_rows, depth), bf16),
        in_specs=[VMEM] * (pairs + 3),
        out_specs=VMEM,
        compiler_params=params(4),
        cost_estimate=COVER,
    )(*blocks, side, limit, partner)
    contexts = exchange([contexts] * pairs)
    part = jax.ShapeDtypeStruct((layers, sequences // 2, columns), f32)
    mine, other = pl.pallas_call(
        functools.partial(pair_project_kernel, pairs, layers, 16 * depth),
        out_shape=(part, part),
        in_specs=[VMEM] * (pairs + 1),
        out_specs=(VMEM, VMEM),
        scratch_shapes=[pltpu.VMEM((sequences * query_rows, depth), f32)],
        compiler_params=params(24),
    )(*contexts, out_proj)
    arrived = lax.ppermute(other, "head", [(0, 1), (1, 0)])
    return (mine + arrived).astype(bf16)


def by_all_to_all(
    queries,
    new_keys,
    token_value_rows,
    cache_keys,
    prefill_value_cache,
    lengths,
    slot_index,
    out_proj,
):
    layers, _, heads, depth = queries.shape
    kv_heads = new_keys.shape[2]
    _, sequences, positions, _, _ = cache_keys.shape
    columns = out_proj.shape[2]
    bf16, f32 = jnp.bfloat16, jnp.float32
    flat = (layers, sequences, positions * kv_heads, depth)
    block = layers * positions * kv_heads
    picked = pl.pallas_call(
        pick_kernel,
        out_shape=jax.ShapeDtypeStruct((sequences, 2, block, depth), bf16),
        in_specs=[SMEM, ANY, ANY],
        out_specs=VMEM,
        scratch_shapes=[pltpu.SemaphoreType.DMA],
        compiler_params=pltpu.CompilerParams(vmem_limit_bytes=8 * 2**20),
    )(slot_index, cache_keys.reshape(flat), prefill_value_cache.reshape(flat))
    gathered = lax.all_to_all(picked, "seq", 0, 0, tiled=True)
    contexts = pl.pallas_call(
        functools.partial(attend_kernel, layers, kv_heads),
        out_shape=jax.ShapeDtypeStruct((sequences, layers * heads, depth), bf16),
        in_specs=[SMEM, VMEM, VMEM, VMEM, VMEM],
        out_specs=VMEM,
        compiler_params=pltpu.CompilerParams(vmem_limit_bytes=24 * 2**20),
    )(
        lengths,
        gathered,
        queries.reshape(layers * heads, depth),
        new_keys.reshape(layers * kv_heads, depth),
        token_value_rows.reshape(layers * kv_heads, depth),
    )
    contexts = lax.all_to_all(contexts, "seq", 0, 0, tiled=True)
    half = sequences // lax.axis_size("head")
    chunk = 4 * depth
    part = jax.ShapeDtypeStruct((layers, half, columns), f32)
    mine, other = pl.pallas_call(
        functools.partial(project_kernel, chunk),
        out_shape=(part, part),
        in_specs=[SMEM, VMEM, ANY],
        out_specs=(VMEM, VMEM),
        scratch_shapes=[
            pltpu.VMEM((sequences * layers * heads, depth), f32),
            pltpu.VMEM(out_proj.shape, bf16),
            pltpu.SemaphoreType.DMA((layers, heads * depth // chunk)),
        ],
        compiler_params=pltpu.CompilerParams(vmem_limit_bytes=40 * 2**20),
    )(lax.axis_index("head").reshape(1), contexts, out_proj)
    arrived = lax.ppermute(other, "head", [(0, 1), (1, 0)])
    return (mine + arrived).astype(bf16)


def solution(mesh):
    placed = (
        P(None, ("grp", "seq"), "head", None),
        P(None, ("grp", "seq"), "head", None),
        P(None, ("grp", "seq"), "head", None),
        P(None, "grp", "seq", "head", None),
        P(None, "grp", "seq", "head", None),
        P(("grp", "seq")),
        P("grp"),
        P(None, "head", "seq"),
    )
    seq = mesh.shape["seq"]
    few = seq in (2, 4, 8)

    def step(*operands):
        return (by_pairs if few else by_all_to_all)(*operands)

    step = jax.shard_map(
        step,
        mesh=mesh,
        in_specs=placed,
        out_specs=P(None, ("grp", "head"), "seq"),
        check_vma=False,
    )
    return step
```
